32 devices in a mesh: rep: 1 (over z), col: 4 (over y), row: 8 (over x, core).
Axes of the slice: x: 4, y: 4, z: 1, core: 2. Of those that a mesh axis runs over, the one named last changes fastest.
The devices are a block of a 4x4x8 slice.
Arguments:
- hidden_0: bfloat16 [128, 3072], P('rep', 'row')
- hidden_1: bfloat16 [128, 3072], P('rep', 'row')
- positions: int32 [128], P(('rep', 'row'))
- lengths: int32 [128], P(('rep', 'row'))
- cache_k: bfloat16 [2, 128, 512, 8, 128], P(None, ('rep', 'row'), None, 'col')
- cache_v: bfloat16 [2, 128, 512, 8, 128], P(None, ('rep', 'row'), None, 'col')
- norm_attn: bfloat16 [2, 3072], P(None, 'row')
- norm_mlp: bfloat16 [2, 3072], P(None, 'row')
- w_query: bfloat16 [2, 3072, 3072], P(None, 'row', 'col')
- w_key: bfloat16 [2, 3072, 1024], P(None, 'row', 'col')
- w_value: bfloat16 [2, 3072, 1024], P(None, 'row', 'col')
- w_out: bfloat16 [2, 3072, 3072], P(None, 'row', 'col')
- w_gate: bfloat16 [2, 3072, 8192], P(None, 'row', 'col')
- w_up: bfloat16 [2, 3072, 8192], P(None, 'row', 'col')
- w_down: bfloat16 [2, 8192, 3072], P(None, 'row', 'col')
Outputs:
- output 1: bfloat16 [128, 3072], P('rep', 'row')
- output 2: bfloat16 [128, 3072], P('rep', 'row')
- output 3: bfloat16 [2, 128, 512, 8, 128], P(None, ('rep', 'row'), None, 'col')
- output 4: bfloat16 [2, 128, 512, 8, 128], P(None, ('rep', 'row'), None, 'col')
All inputs are finite; a program needn't handle non-finite values.
Results may differ from the reference program's by a relative error of at most 0.02.
Values are sent between devices in bfloat16 or wider.
A program may use at most 768 MiB of HBM per device.

```python
import math
import jax
import jax.numpy as jnp
from jax import lax

BATCH = 128
CTX_LEN = 512
D_MODEL = 3072
HEADS = 24
KV_HEADS = 8
HEAD_DIM = 128
FF_DIM = 8192
LAYERS = 2
ROPE_BASE = 1000000
EPS = 1e-05
GROUP_SIZE = HEADS // KV_HEADS
Q_WIDTH = HEADS * HEAD_DIM
KV_WIDTH = KV_HEADS * HEAD_DIM
LEN_BITS = int(math.log2(CTX_LEN))


def draw_lengths(key):
    key_exp, key_len, key_pick, key_pos = jax.random.split(key, 4)
    exponent = jax.random.randint(key_exp, (BATCH,), 0, LEN_BITS + 1)
    length_cap = jnp.minimum(jnp.left_shift(jnp.ones((BATCH,), jnp.int32), exponent), CTX_LEN - 2)
    lengths = 1 + jax.random.randint(key_len, (BATCH,), 0, length_cap)
    shuffled = jax.random.permutation(key_pick, BATCH)
    lengths = lengths.at[shuffled[0]].set(CTX_LEN - 2).at[shuffled[1]].set(1)
    positions = lengths + jax.random.randint(key_pos, (BATCH,), 0, CTX_LEN)
    return positions.astype(jnp.int32), lengths.astype(jnp.int32)


def normal_weight(key, shape, fan_in):
    return (jax.random.normal(key, shape, jnp.float32) * fan_in ** -0.5).astype(jnp.bfloat16)


def setup_inputs(seed: int = 0, part: int = 0) -> dict:
    part_keys = jax.random.split(jax.random.fold_in(jax.random.key(seed), part), 5)
    weight_keys = jax.random.split(jax.random.key(seed + 1), 9)
    positions, lengths = draw_lengths(part_keys[0])
    cache_shape = (LAYERS, BATCH, CTX_LEN, KV_HEADS, HEAD_DIM)
    return {
        'hidden_0': jax.random.normal(part_keys[1], (BATCH, D_MODEL), jnp.float32).astype(jnp.bfloat16),
        'hidden_1': jax.random.normal(part_keys[2], (BATCH, D_MODEL), jnp.float32).astype(jnp.bfloat16),
        'positions': positions,
        'lengths': lengths,
        'cache_k': jax.random.normal(part_keys[3], cache_shape, jnp.float32).astype(jnp.bfloat16),
        'cache_v': jax.random.normal(part_keys[4], cache_shape, jnp.float32).astype(jnp.bfloat16),
        'norm_attn': (1.0 + 0.4 * jax.random.normal(weight_keys[0], (LAYERS, D_MODEL), jnp.float32)).astype(jnp.bfloat16),
        'norm_mlp': (1.0 + 0.4 * jax.random.normal(weight_keys[1], (LAYERS, D_MODEL), jnp.float32)).astype(jnp.bfloat16),
        'w_query': normal_weight(weight_keys[2], (LAYERS, D_MODEL, Q_WIDTH), D_MODEL),
        'w_key': normal_weight(weight_keys[3], (LAYERS, D_MODEL, KV_WIDTH), D_MODEL),
        'w_value': normal_weight(weight_keys[4], (LAYERS, D_MODEL, KV_WIDTH), D_MODEL),
        'w_out': normal_weight(weight_keys[5], (LAYERS, Q_WIDTH, D_MODEL), Q_WIDTH),
        'w_gate': normal_weight(weight_keys[6], (LAYERS, D_MODEL, FF_DIM), D_MODEL),
        'w_up': normal_weight(weight_keys[7], (LAYERS, D_MODEL, FF_DIM), D_MODEL),
        'w_down': normal_weight(weight_keys[8], (LAYERS, FF_DIM, D_MODEL), FF_DIM),
    }


def rms_norm(hidden, gain):
    hidden_f = hidden.astype(jnp.float32)
    scale = lax.rsqrt(jnp.mean(hidden_f * hidden_f, axis=-1, keepdims=True) + EPS)
    return (hidden_f * scale * gain.astype(jnp.float32)).astype(jnp.bfloat16)


def matmul_bf16(left, right):
    return jnp.dot(left, right, preferred_element_type=jnp.float32).astype(jnp.bfloat16)


def rope_rotate(vectors, positions):
    half = HEAD_DIM // 2
    inv_freq = jnp.power(jnp.float32(ROPE_BASE), -jnp.arange(half, dtype=jnp.float32) * 2.0 / HEAD_DIM)
    angles = positions.astype(jnp.float32)[:, None, None] * inv_freq
    cosine = jnp.cos(angles)
    sine = jnp.sin(angles)
    first = vectors[..., :half]
    second = vectors[..., half:]
    return jnp.concatenate([first * cosine - second * sine, second * cosine + first * sine], axis=-1).astype(jnp.bfloat16)


def attend_row(row_inputs):
    query, keys, vals, last_slot = row_inputs
    scores = jnp.einsum('kgd,lkd->kgl', query.astype(jnp.float32), keys.astype(jnp.float32)) * (HEAD_DIM ** -0.5)
    valid = jnp.arange(CTX_LEN)[None, None, :] <= last_slot
    probs = jax.nn.softmax(jnp.where(valid, scores, -jnp.inf), axis=-1).astype(jnp.bfloat16)
    return jnp.einsum('kgl,lkd->kgd', probs.astype(jnp.float32), vals.astype(jnp.float32)).astype(jnp.bfloat16)


def decoder_layer(hidden, layer_weights, keys_layer, vals_layer, positions, slots):
    norm_attn, norm_mlp, w_query, w_key, w_value, w_out, w_gate, w_up, w_down = layer_weights
    batch = hidden.shape[0]
    normed = rms_norm(hidden, norm_attn)
    query = rope_rotate(matmul_bf16(normed, w_query).astype(jnp.float32).reshape(batch, HEADS, HEAD_DIM), positions)
    key_new = rope_rotate(matmul_bf16(normed, w_key).astype(jnp.float32).reshape(batch, KV_HEADS, HEAD_DIM), positions)
    value_new = matmul_bf16(normed, w_value).reshape(batch, KV_HEADS, HEAD_DIM)
    rows = jnp.arange(batch)
    keys_layer = keys_layer.at[rows, slots].set(key_new)
    vals_layer = vals_layer.at[rows, slots].set(value_new)
    attended = lax.map(attend_row, (query.reshape(batch, KV_HEADS, GROUP_SIZE, HEAD_DIM), keys_layer, vals_layer, slots))
    attn_out = matmul_bf16(attended.reshape(batch, Q_WIDTH), w_out)
    hidden = (hidden.astype(jnp.float32) + attn_out.astype(jnp.float32)).astype(jnp.bfloat16)
    normed = rms_norm(hidden, norm_mlp)
    gate = matmul_bf16(normed, w_gate).astype(jnp.float32)
    up_proj = matmul_bf16(normed, w_up).astype(jnp.float32)
    activated = (jax.nn.silu(gate) * up_proj).astype(jnp.bfloat16)
    down_out = matmul_bf16(activated, w_down)
    hidden = (hidden.astype(jnp.float32) + down_out.astype(jnp.float32)).astype(jnp.bfloat16)
    return hidden, keys_layer, vals_layer


def run_step(hidden, positions, slots, cache_k, cache_v, weights):
    def layer_body(carry, layer_inputs):
        layer_weights, keys_layer, vals_layer = layer_inputs
        carry, keys_layer, vals_layer = decoder_layer(carry, layer_weights, keys_layer, vals_layer, positions, slots)
        return carry, (keys_layer, vals_layer)
    hidden, caches = lax.scan(layer_body, hidden, (weights, cache_k, cache_v))
    return hidden, caches[0], caches[1]


def reference(hidden_0, hidden_1, positions, lengths, cache_k, cache_v, norm_attn, norm_mlp, w_query, w_key, w_value, w_out, w_gate, w_up, w_down):
    weights = (norm_attn, norm_mlp, w_query, w_key, w_value, w_out, w_gate, w_up, w_down)
    output_0, cache_k, cache_v = run_step(hidden_0, positions, lengths, cache_k, cache_v, weights)
    output_1, cache_k, cache_v = run_step(hidden_1, positions + 1, lengths + 1, cache_k, cache_v, weights)
    return (output_0, output_1, cache_k, cache_v)
```

```python
import functools

import jax
import jax.numpy as jnp
from jax import lax
from jax.experimental import pallas as pl
from jax.experimental.pallas import tpu as pltpu
from jax.sharding import PartitionSpec as P

ROPE_BASE = 1000000.0
EPS = 1e-05
F32 = jnp.float32
BF16 = jnp.bfloat16
STEPS = 2
MESH = pl.DeviceIdType.MESH
NT = (((1,), (1,)), ((), ()))

(X_INIT, GAIN, N_ATTN, QKV, O_COL, O_ROW, OUT, X_MID, N_MLP, GU, A_COL, A_ROW, DOWN, X_END) = range(14)


def decode_kernel(dims, h0, h1, cos_ref, sin_ref, lim_ref, gain_ref, wq_h, wk_h, wv_h, wo_h, wg_h, wu_h, wd_h, ck_h, cv_h,
                  out0, out1, kn_ref, vn_ref,
                  wq, wk, wv, wo, wg, wu, wd, ck, cv,
                  xb, x, gains, ns, nb, sbq, rbq, qs, sn, pn, os, ago, no, sbo, rbo, sbg, rbg, aga, na,
                  ssem, rsem, wsem):
    R, C, L, D = dims['R'], dims['C'], dims['L'], dims['D']
    HD = dims['HD']
    SEQ = h0.shape[0] // R
    TOK = SEQ * STEPS
    ALL = TOK * R
    WB = h0.shape[1]
    QC, KC = wq.shape[-1], wk.shape[-1]
    QH, KH = QC // HD, KC // HD
    G = QH // KH
    FF = wg.shape[-1]
    HALVES = R // C
    SLOTS = ck.shape[2]
    r = lax.axis_index('row')
    c = lax.axis_index('col')
    own = c * HALVES

    pairs = [(wq_h, wq), (wk_h, wk), (wv_h, wv), (ck_h, ck), (cv_h, cv), (wo_h, wo), (wg_h, wg), (wu_h, wu), (wd_h, wd)]

    def fetch(layer, i):
        return pltpu.make_async_copy(pairs[i][0].at[layer], pairs[i][1].at[layer], wsem.at[layer, i])

    def wwait(layer, *which):
        for i in which:
            fetch(layer, i).wait()

    for i in range(len(pairs)):
        fetch(0, i).start()

    barrier = pltpu.get_barrier_semaphore()
    for j in range(1, R):
        pl.semaphore_signal(barrier, inc=1, device_id={'row': lax.rem(r + j, R)}, device_id_type=MESH)
    for j in range(1, C):
        pl.semaphore_signal(barrier, inc=1, device_id={'col': lax.rem(c + j, C)}, device_id_type=MESH)

    def row_send(ph, src, dst):
        cps = []
        for j in range(1, R):
            peer = lax.rem(r + j, R)
            cp = pltpu.make_async_remote_copy(src_ref=src(peer), dst_ref=dst(j), send_sem=ssem.at[ph, j - 1],
                                              recv_sem=rsem.at[ph, j - 1], device_id={'row': peer}, device_id_type=MESH)
            cp.start()
            cps.append(cp)
        return cps

    def col_send(ph, src, dst):
        cps = []
        for j in range(1, C):
            peer = lax.rem(c + j, C)
            cp = pltpu.make_async_remote_copy(src_ref=src, dst_ref=dst, send_sem=ssem.at[ph, j - 1],
                                              recv_sem=rsem.at[ph, j - 1], device_id={'col': peer}, device_id_type=MESH)
            cp.start()
            cps.append(cp)
        return cps

    def finish(cps):
        for cp in cps:
            cp.wait_recv()
        for cp in cps:
            cp.wait_send()

    def norm(gi, last):
        ss = jnp.zeros((TOK, 1), F32)
        for k in range(R):
            xk = x[k].astype(F32)
            ss = ss + jnp.sum(xk * xk, axis=-1, keepdims=True)
        scale = lax.rsqrt(ss / D + EPS)
        for k in range(R):
            xk = x[k].astype(F32)
            n = xk * scale * gains[k, pl.ds(gi, 1), :]
            if last is not None:
                n = jnp.where(last, xk, n)
            ns[k] = n.astype(BF16)

    def spread(ph, src, dst):
        cps = row_send(ph, lambda peer: src.at[peer], lambda j: dst.at[r])
        dst[r] = src[r]
        finish(cps)

    for b in range(R):
        xb[b, 0:SEQ] = h0[b * SEQ:(b + 1) * SEQ]
        xb[b, SEQ:TOK] = h1[b * SEQ:(b + 1) * SEQ]
    qs[...] = jnp.zeros_like(qs)
    kn_ref[...] = jnp.zeros_like(kn_ref)
    vn_ref[...] = jnp.zeros_like(vn_ref)
    pl.semaphore_wait(barrier, R + C - 2)
    cps = row_send(X_INIT, lambda peer: xb.at[peer], lambda j: x.at[r])
    cps = cps + row_send(GAIN, lambda peer: gain_ref, lambda j: gains.at[r])
    x[r] = xb[r]
    gains[r] = gain_ref[...]
    finish(cps)
    for layer in range(1, L):
        for i in range(len(pairs)):
            fetch(layer, i).start()
    norm(0, None)
    spread(N_ATTN, ns, nb)

    def layer_body(l, carry):
        wwait(l, 0, 1, 2)
        n = nb[...].reshape(ALL, WB)
        col = 0
        for w, width in ((wq, QC), (wk, KC), (wv, KC)):
            res = jnp.dot(n, w[l], preferred_element_type=F32).astype(BF16)
            sbq[:, :, col:col + width] = res.reshape(R, TOK, width)
            col += width
        cps = row_send(QKV, lambda peer: sbq.at[peer], lambda j: rbq.at[j - 1])
        finish(cps)

        cos = cos_ref[...]
        sin = sin_ref[...]

        def head(i):
            sl = slice(i * HD, (i + 1) * HD)
            a = sbq[r, :, sl].astype(F32)
            for j in range(R - 1):
                a = a + rbq[j, :, sl].astype(F32)
            return a.astype(BF16).astype(F32)

        def rope(v):
            return (v * cos + pltpu.roll(v, HD // 2, 1) * sin).astype(BF16).astype(F32)

        for h in range(QH):
            v = rope(head(h))
            for s in range(STEPS):
                qs[:, s * 8 + h, :] = v[s * SEQ:(s + 1) * SEQ]
        for h in range(KH):
            v = rope(head(QH + h))
            w = head(QH + KH + h)
            for s in range(STEPS):
                kn_ref[l, :, s * KH + h, :] = v[s * SEQ:(s + 1) * SEQ]
                vn_ref[l, :, s * KH + h, :] = w[s * SEQ:(s + 1) * SEQ]

        rows = SEQ * 16
        qall = qs[...].reshape(rows, HD).astype(BF16)
        knew = kn_ref[l].reshape(SEQ * 8, HD).astype(BF16)
        vnew = vn_ref[l].reshape(SEQ * 8, HD).astype(BF16)
        sc = HD ** -0.5
        ri = lax.broadcasted_iota(jnp.int32, (rows, SEQ * 8), 0)
        ci = lax.broadcasted_iota(jnp.int32, (rows, SEQ * 8), 1)
        slot = ci % 8
        kvh = jnp.where(ri % 8 >= G, 1, 0)
        ok = (ri // 16 == ci // 8) & (slot < STEPS * KH) & (slot % KH == kvh) & (slot // KH <= (ri % 16) // 8)
        s_new = lax.dot_general(qall, knew, NT, preferred_element_type=F32) * sc
        sn[...] = jnp.where(ok, s_new, -jnp.inf).reshape(SEQ, 16, SEQ * 8)
        wwait(l, 3, 4)
        kvrow = jnp.where(lax.broadcasted_iota(jnp.int32, (16, SLOTS), 0) % 8 >= G, 1, 0)
        kcol = lax.broadcasted_iota(jnp.int32, (16, SLOTS), 1)
        parity = (kcol % KH) == kvrow

        def attend(b, carry):
            s = lax.dot_general(qs[b].astype(BF16), ck[l, b], NT, preferred_element_type=F32) * sc
            s = jnp.where(parity & (kcol < lim_ref[b]), s, -jnp.inf)
            t = sn[b]
            m = jnp.maximum(jnp.max(s, axis=-1, keepdims=True), jnp.max(t, axis=-1, keepdims=True))
            e = jnp.exp(s - m)
            f = jnp.exp(t - m)
            den = jnp.sum(e, axis=-1, keepdims=True) + jnp.sum(f, axis=-1, keepdims=True)
            pn[b] = (f / den).astype(BF16)
            os[b] = jnp.dot((e / den).astype(BF16), cv[l, b], preferred_element_type=F32)
            return carry

        lax.fori_loop(0, SEQ, attend, 0, unroll=2)
        o_new = jnp.dot(pn[...].reshape(rows, SEQ * 8), vnew, preferred_element_type=F32)
        os[...] = os[...] + o_new.reshape(SEQ, 16, HD)
        per = QH // HALVES
        for h in range(QH):
            for s in range(STEPS):
                ago[own + h // per, s * SEQ:(s + 1) * SEQ, (h % per) * HD:(h % per + 1) * HD] = os[:, s * 8 + h, :].astype(BF16)
        mine = pl.ds(own, HALVES)
        finish(col_send(O_COL, ago.at[mine], ago.at[mine]))
        spread(O_ROW, ago, no)

        def project(act, w, depth):
            lhs = act[...].reshape(ALL, depth)
            for h in range(HALVES):
                res = jnp.dot(lhs, w[l, :, h * WB:(h + 1) * WB], preferred_element_type=F32).astype(BF16)
                sbo[:, h] = res.reshape(R, TOK, WB)

        def residual(ph, ph_col):
            finish(row_send(ph, lambda peer: sbo.at[peer], lambda j: rbo.at[j - 1]))
            for h in range(HALVES):
                a = sbo[r, h].astype(F32)
                for j in range(R - 1):
                    a = a + rbo[j, h].astype(F32)
                x[own + h] = (x[own + h].astype(F32) + a.astype(BF16).astype(F32)).astype(BF16)
            finish(col_send(ph_col, x.at[mine], x.at[mine]))

        wwait(l, 5)
        project(no, wo, WB)
        residual(OUT, X_MID)
        norm(L + l, None)
        spread(N_MLP, ns, nb)

        wwait(l, 6, 7)
        tile = FF // 4

        def gate_up(t, carry):
            off = pl.multiple_of(t * tile, tile)
            n = nb[...].reshape(ALL, WB)
            for k, w in enumerate((wg, wu)):
                res = jnp.dot(n, w[l, :, pl.ds(off, tile)], preferred_element_type=F32).astype(BF16)
                sbg[:, :, pl.ds(off + k * FF, tile)] = res.reshape(R, TOK, tile)
            return carry

        lax.fori_loop(0, 4, gate_up, 0)
        finish(row_send(GU, lambda peer: sbg.at[peer], lambda j: rbg.at[j - 1]))
        at = FF // 8
        half = FF // HALVES

        def act(t, carry):
            off = pl.multiple_of(t * at, at)

            def total(base):
                sl = pl.ds(base + off, at)
                a = sbg[r, :, sl].astype(F32)
                for j in range(R - 1):
                    a = a + rbg[j, :, sl].astype(F32)
                return a.astype(BF16).astype(F32)

            g = total(0)
            u = total(FF)
            per_half = half // at
            aga[own + t // per_half, :, pl.ds(pl.multiple_of((t % per_half) * at, at), at)] = (jax.nn.silu(g) * u).astype(BF16)
            return carry

        lax.fori_loop(0, 8, act, 0)
        finish(col_send(A_COL, aga.at[mine], aga.at[mine]))
        spread(A_ROW, aga, na)
        wwait(l, 8)
        project(na, wd, half)
        residual(DOWN, X_END)
        norm(l + 1, l == L - 1)
        spread(N_ATTN, ns, nb)
        return carry

    lax.fori_loop(0, L, layer_body, 0)
    for b in range(R):
        out0[b * SEQ:(b + 1) * SEQ] = nb[b, 0:SEQ]
        out1[b * SEQ:(b + 1) * SEQ] = nb[b, SEQ:TOK]


def cache_kernel(len_ref, kn_ref, vn_ref, ck_ref, cv_ref, ok_ref, ov_ref):
    b = pl.program_id(1)
    rows = ck_ref.shape[2]
    new = STEPS * 2
    start = 2 * len_ref[b]
    base = pl.multiple_of(jnp.minimum((start // 16) * 16, rows - 32), 16)
    win = pl.ds(base, 32)
    idx = lax.broadcasted_iota(jnp.int32, (32, ck_ref.shape[3]), 0) + base - start
    for src, fresh, dst in ((ck_ref, kn_ref, ok_ref), (cv_ref, vn_ref, ov_ref)):
        dst[...] = src[...]
        val = src[0, 0, win, :].astype(F32)
        for i in range(new):
            val = jnp.where(idx == i, fresh[0, 0, i:i + 1, :], val)
        dst[0, 0, win, :] = val.astype(BF16)


def solution(mesh):
    R, C = mesh.shape['row'], mesh.shape['col']
    hidden_spec = P('rep', 'row')
    index_spec = P(('rep', 'row'))
    cache_spec = P(None, ('rep', 'row'), None, 'col', None)
    gain_spec = P(None, 'row')
    weight_spec = P(None, 'row', 'col')

    def device_program(hidden_0, hidden_1, positions, lengths, cache_k, cache_v, norm_attn, norm_mlp, w_query, w_key, w_value, w_out, w_gate, w_up, w_down):
        L, SEQ, CTX, KH, HD = cache_k.shape
        WB = hidden_0.shape[1]
        TOK = SEQ * STEPS
        QC, KC, FF = w_query.shape[-1], w_key.shape[-1], w_gate.shape[-1]
        HALVES = R // C
        SLOTS = CTX * KH
        inv_freq = jnp.power(jnp.float32(ROPE_BASE), -jnp.arange(HD // 2, dtype=F32) * 2.0 / HD)
        pos = jnp.concatenate([positions + s for s in range(STEPS)])
        angles = pos.astype(F32)[:, None] * inv_freq
        cosine, sine = jnp.cos(angles), jnp.sin(angles)
        cos2 = jnp.concatenate([cosine, cosine], axis=1)
        sin2 = jnp.concatenate([-sine, sine], axis=1)
        lim = jnp.broadcast_to((lengths * KH)[:, None, None], (SEQ, 16, 1))
        gain = jnp.concatenate([norm_attn, norm_mlp, jnp.zeros((8 - 2 * L, WB), BF16)]).astype(F32)
        ck = cache_k.reshape(L, SEQ, SLOTS, HD)
        cv = cache_v.reshape(L, SEQ, SLOTS, HD)
        vm = pl.BlockSpec(memory_space=pltpu.VMEM)
        hbm = pl.BlockSpec(memory_space=pl.ANY)
        weights = (w_query, w_key, w_value, w_out, w_gate, w_up, w_down)
        scratch = [pltpu.VMEM(w.shape, BF16) for w in weights] + [pltpu.VMEM(ck.shape, BF16)] * 2
        scratch += [pltpu.VMEM(s, d) for s, d in (
            ((R, TOK, WB), BF16), ((R, TOK, WB), BF16), ((R, 8, WB), F32), ((R, TOK, WB), BF16), ((R, TOK, WB), BF16),
            ((R, TOK, QC + 2 * KC), BF16), ((R - 1, TOK, QC + 2 * KC), BF16),
            ((SEQ, 16, HD), F32), ((SEQ, 16, SEQ * 8), F32), ((SEQ, 16, SEQ * 8), BF16), ((SEQ, 16, HD), F32),
            ((R, TOK, WB), BF16), ((R, TOK, WB), BF16),
            ((R, HALVES, TOK, WB), BF16), ((R - 1, HALVES, TOK, WB), BF16),
            ((R, TOK, 2 * FF), BF16), ((R - 1, TOK, 2 * FF), BF16),
            ((R, TOK, FF // HALVES), BF16), ((R, TOK, FF // HALVES), BF16))]
        scratch += [pltpu.SemaphoreType.DMA((14, R - 1)), pltpu.SemaphoreType.DMA((14, R - 1)), pltpu.SemaphoreType.DMA((L, 9))]
        dims = dict(R=R, C=C, L=L, D=WB * R, HD=HD)
        out_0, out_1, k_new, v_new = pl.pallas_call(
            functools.partial(decode_kernel, dims),
            out_shape=(jax.ShapeDtypeStruct(hidden_0.shape, BF16), jax.ShapeDtypeStruct(hidden_1.shape, BF16),
                       jax.ShapeDtypeStruct((L, SEQ, 8, HD), F32), jax.ShapeDtypeStruct((L, SEQ, 8, HD), F32)),
            in_specs=[vm] * 6 + [hbm] * 9,
            out_specs=(vm, vm, vm, vm),
            scratch_shapes=scratch,
            compiler_params=pltpu.CompilerParams(collective_id=0, has_side_effects=True, vmem_limit_bytes=62 * 1024 * 1024),
            name='decode',
        )(hidden_0, hidden_1, cos2, sin2, lim, gain, *weights, ck, cv)

        block = pl.BlockSpec((1, 1, SLOTS, HD), lambda l, b, n: (l, b, 0, 0))
        fresh = pl.BlockSpec((1, 1, 8, HD), lambda l, b, n: (l, b, 0, 0))
        ok, ov = pl.pallas_call(
            cache_kernel,
            out_shape=(jax.ShapeDtypeStruct(ck.shape, BF16),) * 2,
            grid_spec=pltpu.PrefetchScalarGridSpec(num_scalar_prefetch=1, grid=(L, SEQ), in_specs=[fresh, fresh, block, block],
                                                   out_specs=(block, block)),
            name='cache_update',
        )(lengths, k_new, v_new, ck, cv)
        return out_0, out_1, ok.reshape(cache_k.shape), ov.reshape(cache_v.shape)

    return jax.shard_map(device_program, mesh=mesh,
                         in_specs=(hidden_spec, hidden_spec, index_spec, index_spec, cache_spec, cache_spec, gain_spec, gain_spec) + (weight_spec,) * 7,
                         out_specs=(hidden_spec, hidden_spec, cache_spec, cache_spec), check_vma=False)
```

```python
import functools

import jax
import jax.numpy as jnp
from jax import lax
from jax.experimental import pallas as pl
from jax.experimental.pallas import tpu as pltpu
from jax.sharding import PartitionSpec as P

ROPE_BASE = 1000000.0
EPS = 1e-05
F32 = jnp.float32
BF16 = jnp.bfloat16
STEPS = 2
MESH = pl.DeviceIdType.MESH
NT = (((1,), (1,)), ((), ()))

CORES = 2
COPY_GROUPS = 4
STREAMS = 2

(X_INIT, GAIN, N_ATTN, QKV_A, QKV_B, O_COL, O_ROW, OUT_A, OUT_B, X_MID, N_MLP, GU_A, GU_B, A_COL, A_ROW, DOWN_A, DOWN_B,
 X_END, PHASES) = range(19)
PRE = {QKV_B: QKV_A, GU_B: GU_A, OUT_B: None, DOWN_B: None}


def decode_kernel(dims, h0, h1, cos_ref, sin_ref, lim_ref, gain_ref, wq_h, wk_h, wv_h, wo_h, wg_h, wu_h, wd_h, ck_h, cv_h,
                  out0, out1, kn_ref, vn_ref,
                  wq, wk, wv, wo, wg, wu, wd, ck, cv,
                  xb, x, gains, ns, nb, sbq, prq, rbq, qs, sn, pn, os, ago, no, sbo, pro, rbo, sbg, prg, rbg, aga, na,
                  ssem, rsem, wsem):
    R, C, L, D = dims['R'], dims['C'], dims['L'], dims['D']
    HD = dims['HD']
    SEQ = h0.shape[0] // R
    SZ = SEQ // STREAMS
    TOK = SZ * STEPS
    ALL = TOK * R
    WB = h0.shape[1]
    QC, KC = wq.shape[-1], wk.shape[-1]
    QH, KH = QC // HD, KC // HD
    G = QH // KH
    FF = wg.shape[-1]
    HALVES = R // C
    SLOTS = ck.shape[2]
    XS = R // CORES
    r = lax.axis_index('row')
    c = lax.axis_index('col')
    chip, core = lax.div(r, CORES), lax.rem(r, CORES)
    own = c * HALVES
    mine = pl.ds(own, HALVES)

    pairs = [(wq_h, wq), (wk_h, wk), (wv_h, wv), (ck_h, ck), (cv_h, cv), (wo_h, wo), (wg_h, wg), (wu_h, wu), (wd_h, wd)]

    def fetch(layer, i):
        return pltpu.make_async_copy(pairs[i][0].at[layer], pairs[i][1].at[layer], wsem.at[layer, i])

    def wwait(layer, *which):
        for i in which:
            fetch(layer, i).wait()

    for i in range(len(pairs)):
        fetch(0, i).start()

    barrier = pltpu.get_barrier_semaphore()
    for j in range(1, R):
        pl.semaphore_signal(barrier, inc=1, device_id={'row': lax.rem(r + j, R)}, device_id_type=MESH)
    for j in range(1, C):
        pl.semaphore_signal(barrier, inc=1, device_id={'col': lax.rem(c + j, C)}, device_id_type=MESH)

    def remote(ph, z, j, src, dst, device):
        return pltpu.make_async_remote_copy(src_ref=src, dst_ref=dst, send_sem=ssem.at[ph, z, j], recv_sem=rsem.at[ph, z, j],
                                            device_id=device, device_id_type=MESH)

    def row_copies(ph, z, src, dst):
        for j in range(1, R):
            peer = lax.rem(r + j, R)
            yield remote(ph, z, j - 1, src(peer), dst(j), {'row': peer})

    def chip_copies(ph, z, src, dst):
        for j in range(1, XS):
            peer = lax.rem(chip + j, XS)
            yield remote(ph, z, j - 1, src(peer), dst(j), {'row': peer * CORES + core})

    def col_copies(ph, z, src, dst):
        for j in range(1, C):
            yield remote(ph, z, j - 1, src, dst, {'col': lax.rem(c + j, C)})

    def core_copies(ph, z, src, dst):
        yield remote(ph, z, 0, src, dst, {'row': r + 1 - 2 * core})

    def start(copies):
        for cp in copies:
            cp.start()

    def finish(copies):
        cps = list(copies)
        for cp in cps:
            cp.wait_recv()
        for cp in cps:
            cp.wait_send()

    def spread(ph, z, src, dst):
        return row_copies(ph, z, lambda peer: src.at[z, peer], lambda j: dst.at[z, r])

    def spread_start(ph, z, src, dst):
        start(spread(ph, z, src, dst))
        dst[z, r] = src[z, r]

    def gather(ph, z, buf):
        return col_copies(ph, z, buf.at[z, mine], buf.at[z, mine])

    def core_sum(ph, z, sb, pr):
        return core_copies(ph, z, sb.at[z, 1 - core], pr.at[z])

    def chip_sum(ph, z, sb, rb):
        return chip_copies(ph, z, lambda peer: sb.at[z, core, peer], lambda j: rb.at[z, j - 1])

    def row_sum(ph, z, sb, rb):
        return row_copies(ph, z, lambda peer: sb.at[z, lax.rem(peer, CORES), lax.div(peer, CORES)], lambda j: rb.at[z, j - 1])

    def sum_start(ph, z, sb, pr, rb):
        start(core_sum(PRE[ph], z, sb, pr) if PRE[ph] is not None else row_sum(ph, z, sb, rb))

    def sum_middle(ph, z, sb, pr, rb, tiles):
        if PRE[ph] is None:
            return
        finish(core_sum(PRE[ph], z, sb, pr))
        width = sb.shape[-1] // tiles

        def add(t, carry):
            sl = pl.ds(pl.multiple_of(t * width, width), width)
            sb[z, core, :, :, sl] = (sb[z, core, :, :, sl].astype(F32) + pr[z, :, :, sl].astype(F32)).astype(BF16)
            return carry

        lax.fori_loop(0, tiles, add, 0)
        start(chip_sum(ph, z, sb, rb))

    def sum_finish(ph, z, sb, rb):
        finish(chip_sum(ph, z, sb, rb) if PRE[ph] is not None else row_sum(ph, z, sb, rb))

    def total(ph, z, sb, rb, sl):
        a = sb[z, core, chip, :, sl].astype(F32)
        for j in range((XS if PRE[ph] is not None else R) - 1):
            a = a + rb[z, j, :, sl].astype(F32)
        return a.astype(BF16).astype(F32)

    def put(sb, z, cols, res):
        v = res.astype(BF16).reshape(XS, CORES, TOK, res.shape[-1])
        for k in range(CORES):
            sb[z, k, :, :, cols] = v[:, k]

    def norm(z, gi, last):
        ss = jnp.zeros((TOK, 1), F32)
        for k in range(R):
            xk = x[z, k].astype(F32)
            ss = ss + jnp.sum(xk * xk, axis=-1, keepdims=True)
        scale = lax.rsqrt(ss / D + EPS)
        for k in range(R):
            xk = x[z, k].astype(F32)
            n = xk * scale * gains[k, pl.ds(gi, 1), :]
            if last is not None:
                n = jnp.where(last, xk, n)
            ns[z, k] = n.astype(BF16)

    for b in range(R):
        v0 = h0[b * SEQ:(b + 1) * SEQ].astype(F32)
        v1 = h1[b * SEQ:(b + 1) * SEQ].astype(F32)
        for z in range(STREAMS):
            part = slice(z * SZ, (z + 1) * SZ)
            xb[z, b] = jnp.concatenate([v0[part], v1[part]], axis=0).astype(BF16)
    qs[...] = jnp.zeros_like(qs)
    kn_ref[...] = jnp.zeros_like(kn_ref)
    vn_ref[...] = jnp.zeros_like(vn_ref)
    pl.semaphore_wait(barrier, R + C - 2)

    def gain_copies():
        return row_copies(GAIN, 0, lambda peer: gain_ref, lambda j: gains.at[r])

    for z in range(STREAMS):
        spread_start(X_INIT, z, xb, x)
        if z == 0:
            start(gain_copies())
    gains[r] = gain_ref[...]
    for layer in range(1, L):
        for i in range(len(pairs)):
            fetch(layer, i).start()
    for z in range(STREAMS):
        finish(spread(X_INIT, z, xb, x))
        if z == 0:
            finish(gain_copies())
        norm(z, 0, None)
        spread_start(N_ATTN, z, ns, nb)

    rows = SZ * 16
    sc = HD ** -0.5
    ri = lax.broadcasted_iota(jnp.int32, (rows, SZ * 8), 0)
    ci = lax.broadcasted_iota(jnp.int32, (rows, SZ * 8), 1)
    slot = ci % 8
    kvh = jnp.where(ri % 8 >= G, 1, 0)
    new_ok = (ri // 16 == ci // 8) & (slot < STEPS * KH) & (slot % KH == kvh) & (slot // KH <= (ri % 16) // 8)
    per = QH // HALVES
    tile = FF // 4
    half = FF // HALVES

    def layer_body(l, carry):
        def qkv(z):
            finish(spread(N_ATTN, z, ns, nb))
            if z == 0:
                wwait(l, 0, 1, 2)
            n = nb[z].reshape(ALL, WB)
            col = 0
            for w, width in ((wq, QC), (wk, KC), (wv, KC)):
                put(sbq, z, slice(col, col + width), jnp.dot(n, w[l], preferred_element_type=F32))
                col += width
            sum_start(QKV_B, z, sbq, prq, rbq)

        def qkv_middle(z):
            sum_middle(QKV_B, z, sbq, prq, rbq, 2)

        def attention(z):
            sum_finish(QKV_B, z, sbq, rbq)
            cos = cos_ref[z]
            sin = sin_ref[z]

            def head(i):
                return total(QKV_B, z, sbq, rbq, slice(i * HD, (i + 1) * HD))

            def rope(v):
                return (v * cos + pltpu.roll(v, HD // 2, 1) * sin).astype(BF16).astype(F32)

            seqs = slice(z * SZ, (z + 1) * SZ)
            for h in range(QH):
                v = rope(head(h))
                for s in range(STEPS):
                    qs[:, s * 8 + h, :] = v[s * SZ:(s + 1) * SZ]
            for h in range(KH):
                v = rope(head(QH + h))
                w = head(QH + KH + h)
                for s in range(STEPS):
                    kn_ref[l, seqs, s * KH + h, :] = v[s * SZ:(s + 1) * SZ]
                    vn_ref[l, seqs, s * KH + h, :] = w[s * SZ:(s + 1) * SZ]

            qall = qs[...].reshape(rows, HD).astype(BF16)
            knew = kn_ref[l, seqs].reshape(SZ * 8, HD).astype(BF16)
            vnew = vn_ref[l, seqs].reshape(SZ * 8, HD).astype(BF16)
            s_new = lax.dot_general(qall, knew, NT, preferred_element_type=F32) * sc
            sn[...] = jnp.where(new_ok, s_new, -jnp.inf).reshape(SZ, 16, SZ * 8)
            if z == 0:
                wwait(l, 3, 4)
            kvrow = jnp.where(lax.broadcasted_iota(jnp.int32, (16, SLOTS), 0) % 8 >= G, 1, 0)
            kcol = lax.broadcasted_iota(jnp.int32, (16, SLOTS), 1)
            parity = (kcol % KH) == kvrow

            def attend(b, carry):
                q = z * SZ + b
                s = lax.dot_general(qs[b].astype(BF16), ck[l, q], NT, preferred_element_type=F32) * sc
                s = jnp.where(parity & (kcol < lim_ref[q]), s, -jnp.inf)
                t = sn[b]
                m = jnp.maximum(jnp.max(s, axis=-1, keepdims=True), jnp.max(t, axis=-1, keepdims=True))
                e = jnp.exp(s - m)
                f = jnp.exp(t - m)
                den = jnp.sum(e, axis=-1, keepdims=True) + jnp.sum(f, axis=-1, keepdims=True)
                pn[b] = (f / den).astype(BF16)
                os[b] = jnp.dot((e / den).astype(BF16), cv[l, q], preferred_element_type=F32)
                return carry

            lax.fori_loop(0, SZ, attend, 0, unroll=4)
            o_new = jnp.dot(pn[...].reshape(rows, SZ * 8), vnew, preferred_element_type=F32)
            os[...] = os[...] + o_new.reshape(SZ, 16, HD)
            for h in range(QH):
                o = jnp.concatenate([os[:, s * 8 + h, :] for s in range(STEPS)], axis=0)
                ago[z, own + h // per, :, (h % per) * HD:(h % per + 1) * HD] = o.astype(BF16)
            start(gather(O_COL, z, ago))

        def o_row(z):
            finish(gather(O_COL, z, ago))
            spread_start(O_ROW, z, ago, no)

        def project(act, z, w, depth, ph):
            lhs = act[z].reshape(ALL, depth)
            for h in range(HALVES):
                put(sbo, z, slice(h * WB, (h + 1) * WB),
                    jnp.dot(lhs, w[l, :, h * WB:(h + 1) * WB], preferred_element_type=F32))
            sum_start(ph, z, sbo, pro, rbo)

        def out(z):
            finish(spread(O_ROW, z, ago, no))
            if z == 0:
                wwait(l, 5)
            project(no, z, wo, WB, OUT_B)

        def residual(z, ph, ph_col):
            sum_finish(ph, z, sbo, rbo)
            for h in range(HALVES):
                a = total(ph, z, sbo, rbo, slice(h * WB, (h + 1) * WB))
                x[z, own + h] = (x[z, own + h].astype(F32) + a).astype(BF16)
            start(gather(ph_col, z, x))

        def mlp_norm(z):
            finish(gather(X_MID, z, x))
            norm(z, L + l, None)
            spread_start(N_MLP, z, ns, nb)

        def gate_up(z):
            finish(spread(N_MLP, z, ns, nb))
            if z == 0:
                wwait(l, 6, 7)

            def body(t, carry):
                off = pl.multiple_of(t * tile, tile)
                n = nb[z].reshape(ALL, WB)
                for k, w in enumerate((wg, wu)):
                    put(sbg, z, pl.ds(off + k * FF, tile), jnp.dot(n, w[l, :, pl.ds(off, tile)], preferred_element_type=F32))
                return carry

            lax.fori_loop(0, 4, body, 0)
            sum_start(GU_B, z, sbg, prg, rbg)

        def gate_up_middle(z):
            sum_middle(GU_B, z, sbg, prg, rbg, 8)

        def act(z):
            sum_finish(GU_B, z, sbg, rbg)
            per_half = half // tile

            def body(t, carry):
                off = pl.multiple_of(t * tile, tile)
                g = total(GU_B, z, sbg, rbg, pl.ds(off, tile))
                u = total(GU_B, z, sbg, rbg, pl.ds(off + FF, tile))
                aga[z, own + t // per_half, :, pl.ds(pl.multiple_of((t % per_half) * tile, tile), tile)] = (jax.nn.silu(g) * u).astype(BF16)
                return carry

            lax.fori_loop(0, 4, body, 0)
            start(gather(A_COL, z, aga))

        def a_row(z):
            finish(gather(A_COL, z, aga))
            spread_start(A_ROW, z, aga, na)

        def down(z):
            finish(spread(A_ROW, z, aga, na))
            if z == 0:
                wwait(l, 8)
            project(na, z, wd, half, DOWN_B)

        def end_norm(z):
            finish(gather(X_END, z, x))
            norm(z, l + 1, l == L - 1)
            spread_start(N_ATTN, z, ns, nb)

        stages = [qkv, qkv_middle, attention, o_row, out]
        stages += [lambda z: sum_middle(OUT_B, z, sbo, pro, rbo, 1)] if PRE[OUT_B] is not None else []
        stages += [lambda z: residual(z, OUT_B, X_MID), mlp_norm, gate_up, gate_up_middle, act, a_row, down]
        stages += [lambda z: sum_middle(DOWN_B, z, sbo, pro, rbo, 1)] if PRE[DOWN_B] is not None else []
        stages += [lambda z: residual(z, DOWN_B, X_END), end_norm]
        for stage in stages:
            for z in range(STREAMS):
                stage(z)
        return carry

    lax.fori_loop(0, L, layer_body, 0)
    for z in range(STREAMS):
        finish(spread(N_ATTN, z, ns, nb))
    for b in range(R):
        v = [nb[z, b].astype(F32) for z in range(STREAMS)]
        for s, out in enumerate((out0, out1)):
            out[b * SEQ:(b + 1) * SEQ] = jnp.concatenate([w[s * SZ:(s + 1) * SZ] for w in v], axis=0).astype(BF16)


def cache_kernel(heads, len_ref, kn_ref, vn_ref, ck_ref, cv_ref, ok_ref, ov_ref, kbuf, vbuf, rsem, wsem):
    layers, seqs, rows, width = ck_ref.shape
    group = seqs // COPY_GROUPS
    sides = ((ck_ref, kbuf, kn_ref, ok_ref), (cv_ref, vbuf, vn_ref, ov_ref))

    def load(k, i):
        at = (i // COPY_GROUPS, pl.ds((i % COPY_GROUPS) * group, group))
        return pltpu.make_async_copy(sides[k][0].at[at], sides[k][1].at[i], rsem.at[k, i])

    def save(k, i):
        at = (i // COPY_GROUPS, pl.ds((i % COPY_GROUPS) * group, group))
        return pltpu.make_async_copy(sides[k][1].at[i], sides[k][3].at[at], wsem.at[k, i])

    count = layers * COPY_GROUPS
    for i in range(count):
        for k in range(2):
            load(k, i).start()
    for i in range(count):
        layer, first = i // COPY_GROUPS, (i % COPY_GROUPS) * group
        for k in range(2):
            load(k, i).wait()

            def patch(g, carry):
                buf, fresh = sides[k][1], sides[k][2]
                at = len_ref[first + g] * heads
                base = pl.multiple_of(jnp.minimum((at // 16) * 16, rows - 32), 16)
                win = pl.ds(base, 32)
                idx = lax.broadcasted_iota(jnp.int32, (32, width), 0) + base - at
                val = buf[i, g, win, :].astype(F32)
                new = fresh[layer, first + g]
                for n in range(STEPS * heads):
                    val = jnp.where(idx == n, new[n:n + 1, :], val)
                buf[i, g, win, :] = val.astype(BF16)
                return carry

            lax.fori_loop(0, group, patch, 0, unroll=True)
            save(k, i).start()
    for i in range(count):
        for k in range(2):
            save(k, i).wait()


def solution(mesh):
    R, C = mesh.shape['row'], mesh.shape['col']
    hidden_spec = P('rep', 'row')
    index_spec = P(('rep', 'row'))
    cache_spec = P(None, ('rep', 'row'), None, 'col', None)
    gain_spec = P(None, 'row')
    weight_spec = P(None, 'row', 'col')

    def device_program(hidden_0, hidden_1, positions, lengths, cache_k, cache_v, norm_attn, norm_mlp, w_query, w_key, w_value, w_out, w_gate, w_up, w_down):
        L, SEQ, CTX, KH, HD = cache_k.shape
        WB = hidden_0.shape[1]
        SZ = SEQ // STREAMS
        TOK = SZ * STEPS
        XS = R // CORES
        Z = STREAMS
        QC, KC, FF = w_query.shape[-1], w_key.shape[-1], w_gate.shape[-1]
        HALVES = R // C
        SLOTS = CTX * KH
        inv_freq = jnp.power(jnp.float32(ROPE_BASE), -jnp.arange(HD // 2, dtype=F32) * 2.0 / HD)
        pos = jnp.concatenate([(positions + s).reshape(Z, SZ) for s in range(STEPS)], axis=1)
        angles = pos.astype(F32)[:, :, None] * inv_freq
        cosine, sine = jnp.cos(angles), jnp.sin(angles)
        cos2 = jnp.concatenate([cosine, cosine], axis=2)
        sin2 = jnp.concatenate([-sine, sine], axis=2)
        lim = jnp.broadcast_to((lengths * KH)[:, None, None], (SEQ, 16, 1))
        gain = jnp.concatenate([norm_attn, norm_mlp, jnp.zeros((8 - 2 * L, WB), BF16)]).astype(F32)
        ck = cache_k.reshape(L, SEQ, SLOTS, HD)
        cv = cache_v.reshape(L, SEQ, SLOTS, HD)
        vm = pl.BlockSpec(memory_space=pltpu.VMEM)
        hbm = pl.BlockSpec(memory_space=pl.ANY)
        weights = (w_query, w_key, w_value, w_out, w_gate, w_up, w_down)
        scratch = [pltpu.VMEM(w.shape, BF16) for w in weights] + [pltpu.VMEM(ck.shape, BF16)] * 2
        N3 = QC + 2 * KC
        N2 = 2 * FF
        OUTW = HALVES * WB

        def slots(ph):
            return R - 1 if PRE[ph] is None else XS - 1

        scratch += [pltpu.VMEM(s, d) for s, d in (
            ((Z, R, TOK, WB), BF16), ((Z, R, TOK, WB), BF16), ((R, 8, WB), F32), ((Z, R, TOK, WB), BF16), ((Z, R, TOK, WB), BF16),
            ((Z, CORES, XS, TOK, N3), BF16), ((Z, XS, TOK, N3), BF16), ((Z, slots(QKV_B), TOK, N3), BF16),
            ((SZ, 16, HD), F32), ((SZ, 16, SZ * 8), F32), ((SZ, 16, SZ * 8), BF16), ((SZ, 16, HD), F32),
            ((Z, R, TOK, WB), BF16), ((Z, R, TOK, WB), BF16),
            ((Z, CORES, XS, TOK, OUTW), BF16), ((Z, XS, TOK, OUTW), BF16), ((Z, slots(OUT_B), TOK, OUTW), BF16),
            ((Z, CORES, XS, TOK, N2), BF16), ((Z, XS, TOK, N2), BF16), ((Z, slots(GU_B), TOK, N2), BF16),
            ((Z, R, TOK, FF // HALVES), BF16), ((Z, R, TOK, FF // HALVES), BF16))]
        scratch += [pltpu.SemaphoreType.DMA((PHASES, Z, R - 1))] * 2 + [pltpu.SemaphoreType.DMA((L, 9))]
        dims = dict(R=R, C=C, L=L, D=WB * R, HD=HD)
        out_0, out_1, k_new, v_new = pl.pallas_call(
            functools.partial(decode_kernel, dims),
            out_shape=(jax.ShapeDtypeStruct(hidden_0.shape, BF16), jax.ShapeDtypeStruct(hidden_1.shape, BF16),
                       jax.ShapeDtypeStruct((L, SEQ, 8, HD), F32), jax.ShapeDtypeStruct((L, SEQ, 8, HD), F32)),
            in_specs=[vm] * 6 + [hbm] * 9,
            out_specs=(vm, vm, vm, vm),
            scratch_shapes=scratch,
            compiler_params=pltpu.CompilerParams(collective_id=0, has_side_effects=True, vmem_limit_bytes=62 * 1024 * 1024),
            name='decode',
        )(hidden_0, hidden_1, cos2, sin2, lim, gain, *weights, ck, cv)

        smem = pl.BlockSpec(memory_space=pltpu.SMEM)
        count = L * COPY_GROUPS
        buf = pltpu.VMEM((count, SEQ // COPY_GROUPS, SLOTS, HD), BF16)
        ok, ov = pl.pallas_call(
            functools.partial(cache_kernel, KH),
            out_shape=(jax.ShapeDtypeStruct(ck.shape, BF16),) * 2,
            in_specs=[smem, vm, vm, hbm, hbm],
            out_specs=(hbm, hbm),
            scratch_shapes=[buf, buf, pltpu.SemaphoreType.DMA((2, count)), pltpu.SemaphoreType.DMA((2, count))],
            compiler_params=pltpu.CompilerParams(vmem_limit_bytes=32 * 1024 * 1024),
            name='cache_update',
        )(lengths, k_new, v_new, ck, cv)
        ok, ov = ok.reshape(cache_k.shape), ov.reshape(cache_v.shape)
        return out_0, out_1, ok, ov

    return jax.shard_map(device_program, mesh=mesh,
                         in_specs=(hidden_spec, hidden_spec, index_spec, index_spec, cache_spec, cache_spec, gain_spec, gain_spec) + (weight_spec,) * 7,
                         out_specs=(hidden_spec, hidden_spec, cache_spec, cache_spec), check_vma=False)
```

```python
import functools
import math

import jax
import jax.numpy as jnp
from jax import lax
from jax.experimental import pallas as pl
from jax.experimental.pallas import tpu as pltpu
from jax.sharding import PartitionSpec as P

ROPE_BASE = 1000000.0
EPS = 1e-05
F32 = jnp.float32
BF16 = jnp.bfloat16
STEPS = 2
MESH = pl.DeviceIdType.MESH
NT = (((1,), (1,)), ((), ()))

CORES = 2
COPY_GROUPS = 4
STREAMS = 2

(X_INIT, GAIN, N_ATTN, QKV_A, QKV_B, O_COL, O_ROW, OUT_A, OUT_B, X_MID, N_MLP, GU_A, GU_B, A_COL, A_ROW, DOWN_A, DOWN_B,
 X_END, PHASES) = range(19)
PRE = {QKV_B: None, GU_B: GU_A, OUT_B: None, DOWN_B: None}


def decode_kernel(dims, h0, h1, pos_ref, len_ref, ga_ref, gm_ref, wq_h, wk_h, wv_h, wo_h, wg_h, wu_h, wd_h, ck_h, cv_h,
                  out0, out1, kn_ref, vn_ref,
                  wq, wk, wv, wo, wg, wu, wd, ck, cv,
                  cos_ref, sin_ref, gain_ref, xb, x, gains, ns, nb, sbq, prq, rbq, qs, sn, pn, os, ago, no, sbo, pro, rbo, sbg, prg, rbg, aga, na,
                  ssem, rsem, wsem):
    R, C, L, D = dims['R'], dims['C'], dims['L'], dims['D']
    HD = dims['HD']
    SEQ = h0.shape[0] // R
    SZ = SEQ // STREAMS
    TOK = SZ * STEPS
    ALL = TOK * R
    WB = h0.shape[1]
    QC, KC = wq.shape[-1], wk.shape[-1]
    QH, KH = QC // HD, KC // HD
    G = QH // KH
    FF = wg.shape[-1]
    HALVES = R // C
    SLOTS = ck.shape[2]
    XS = R // CORES
    r = lax.axis_index('row')
    c = lax.axis_index('col')
    chip, core = lax.div(r, CORES), lax.rem(r, CORES)
    own = c * HALVES
    mine = pl.ds(own, HALVES)

    pairs = [(wq_h, wq), (wk_h, wk), (wv_h, wv), (ck_h, ck), (cv_h, cv), (wo_h, wo), (wg_h, wg), (wu_h, wu), (wd_h, wd)]

    def fetch(layer, i):
        return pltpu.make_async_copy(pairs[i][0].at[layer], pairs[i][1].at[layer], wsem.at[layer, i])

    def wwait(layer, *which):
        for i in which:
            fetch(layer, i).wait()

    for i in range(len(pairs)):
        fetch(0, i).start()

    barrier = pltpu.get_barrier_semaphore()
    for j in range(1, R):
        pl.semaphore_signal(barrier, inc=1, device_id={'row': lax.rem(r + j, R)}, device_id_type=MESH)
    for j in range(1, C):
        pl.semaphore_signal(barrier, inc=1, device_id={'col': lax.rem(c + j, C)}, device_id_type=MESH)

    def remote(ph, z, j, src, dst, device):
        return pltpu.make_async_remote_copy(src_ref=src, dst_ref=dst, send_sem=ssem.at[ph, z, j], recv_sem=rsem.at[ph, z, j],
                                            device_id=device, device_id_type=MESH)

    def row_copies(ph, z, src, dst):
        for j in range(1, R):
            peer = lax.rem(r + j, R)
            yield remote(ph, z, j - 1, src(peer), dst(j), {'row': peer})

    def chip_copies(ph, z, src, dst):
        for j in range(1, XS):
            peer = lax.rem(chip + j, XS)
            yield remote(ph, z, j - 1, src(peer), dst(j), {'row': peer * CORES + core})

    def col_copies(ph, z, src, dst):
        for j in range(1, C):
            yield remote(ph, z, j - 1, src, dst, {'col': lax.rem(c + j, C)})

    def core_copies(ph, z, src, dst):
        yield remote(ph, z, 0, src, dst, {'row': r + 1 - 2 * core})

    def start(copies):
        for cp in copies:
            cp.start()

    def finish(copies):
        cps = list(copies)
        for cp in cps:
            cp.wait_recv()
        for cp in cps:
            cp.wait_send()

    def spread(ph, z, src, dst):
        return row_copies(ph, z, lambda peer: src.at[z, peer], lambda j: dst.at[z, r])

    def spread_start(ph, z, src, dst):
        start(spread(ph, z, src, dst))
        dst[z, r] = src[z, r]

    def gather(ph, z, buf):
        return col_copies(ph, z, buf.at[z, mine], buf.at[z, mine])

    def core_sum(ph, z, sb, pr):
        return core_copies(ph, z, sb.at[z, 1 - core], pr.at[z])

    def chip_sum(ph, z, sb, rb):
        return chip_copies(ph, z, lambda peer: sb.at[z, core, peer], lambda j: rb.at[z, j - 1])

    def row_sum(ph, z, sb, rb):
        return row_copies(ph, z, lambda peer: sb.at[z, lax.rem(peer, CORES), lax.div(peer, CORES)], lambda j: rb.at[z, j - 1])

    def sum_start(ph, z, sb, pr, rb):
        start(core_sum(PRE[ph], z, sb, pr) if PRE[ph] is not None else row_sum(ph, z, sb, rb))

    def sum_middle(ph, z, sb, pr, rb, tiles):
        if PRE[ph] is None:
            return
        finish(core_sum(PRE[ph], z, sb, pr))
        width = sb.shape[-1] // tiles

        def add(t, carry):
            sl = pl.ds(pl.multiple_of(t * width, width), width)
            sb[z, core, :, :, sl] = (sb[z, core, :, :, sl].astype(F32) + pr[z, :, :, sl].astype(F32)).astype(BF16)
            return carry

        lax.fori_loop(0, tiles, add, 0)
        start(chip_sum(ph, z, sb, rb))

    def sum_finish(ph, z, sb, rb):
        finish(chip_sum(ph, z, sb, rb) if PRE[ph] is not None else row_sum(ph, z, sb, rb))

    def total(ph, z, sb, rb, sl):
        a = sb[z, core, chip, :, sl].astype(F32)
        for j in range((XS if PRE[ph] is not None else R) - 1):
            a = a + rb[z, j, :, sl].astype(F32)
        return a.astype(BF16).astype(F32)

    def put(sb, z, cols, res):
        v = res.astype(BF16).reshape(XS, CORES, TOK, res.shape[-1])
        for k in range(CORES):
            sb[z, k, :, :, cols] = v[:, k]

    def norm(z, gi, last):
        ss = jnp.zeros((TOK, 1), F32)
        for k in range(R):
            xk = x[z, k].astype(F32)
            ss = ss + jnp.sum(xk * xk, axis=-1, keepdims=True)
        scale = lax.rsqrt(ss / D + EPS)
        for k in range(R):
            xk = x[z, k].astype(F32)
            n = xk * scale * gains[k, pl.ds(gi, 1), :]
            if last is not None:
                n = jnp.where(last, xk, n)
            ns[z, k] = n.astype(BF16)

    gain_ref[...] = jnp.zeros_like(gain_ref)
    gain_ref[0:L] = ga_ref[...].astype(F32)
    gain_ref[L:2 * L] = gm_ref[...].astype(F32)
    lane = lax.broadcasted_iota(jnp.int32, (TOK, HD), 1)
    token = lax.broadcasted_iota(jnp.int32, (TOK, HD), 0)
    half_lane = lax.rem(lane, HD // 2)
    inv_freq = jnp.exp(half_lane.astype(F32) * (-2.0 / HD * math.log(ROPE_BASE)))
    for z in range(STREAMS):
        position = jnp.zeros((TOK, HD), jnp.int32)
        for b in range(SZ):
            position = jnp.where(lax.rem(token, SZ) == b, pos_ref[z * SZ + b], position)
        angle = (position + lax.div(token, SZ)).astype(F32) * inv_freq
        cos_ref[z] = jnp.cos(angle)
        sine = jnp.sin(angle)
        sin_ref[z] = jnp.where(lane < HD // 2, -sine, sine)

    for b in range(R):
        v0 = h0[b * SEQ:(b + 1) * SEQ].astype(F32)
        v1 = h1[b * SEQ:(b + 1) * SEQ].astype(F32)
        for z in range(STREAMS):
            part = slice(z * SZ, (z + 1) * SZ)
            xb[z, b] = jnp.concatenate([v0[part], v1[part]], axis=0).astype(BF16)
    qs[...] = jnp.zeros_like(qs)
    kn_ref[...] = jnp.zeros_like(kn_ref)
    vn_ref[...] = jnp.zeros_like(vn_ref)
    pl.semaphore_wait(barrier, R + C - 2)

    def gain_copies():
        return row_copies(GAIN, 0, lambda peer: gain_ref, lambda j: gains.at[r])

    for z in range(STREAMS):
        spread_start(X_INIT, z, xb, x)
        if z == 0:
            start(gain_copies())
    gains[r] = gain_ref[...]
    for layer in range(1, L):
        for i in range(len(pairs)):
            fetch(layer, i).start()
    for z in range(STREAMS):
        finish(spread(X_INIT, z, xb, x))
        if z == 0:
            finish(gain_copies())
        norm(z, 0, None)
        spread_start(N_ATTN, z, ns, nb)

    rows = SZ * 16
    sc = HD ** -0.5
    ri = lax.broadcasted_iota(jnp.int32, (rows, SZ * 8), 0)
    ci = lax.broadcasted_iota(jnp.int32, (rows, SZ * 8), 1)
    slot = ci % 8
    kvh = jnp.where(ri % 8 >= G, 1, 0)
    new_ok = (ri // 16 == ci // 8) & (slot < STEPS * KH) & (slot % KH == kvh) & (slot // KH <= (ri % 16) // 8)
    per = QH // HALVES
    tile = FF // 4
    half = FF // HALVES

    def layer_body(l, carry):
        def qkv(z):
            finish(spread(N_ATTN, z, ns, nb))
            if z == 0:
                wwait(l, 0, 1, 2)
            n = nb[z].reshape(ALL, WB)
            col = 0
            for w, width in ((wq, QC), (wk, KC), (wv, KC)):
                put(sbq, z, slice(col, col + width), jnp.dot(n, w[l], preferred_element_type=F32))
                col += width
            sum_start(QKV_B, z, sbq, prq, rbq)

        def qkv_middle(z):
            sum_middle(QKV_B, z, sbq, prq, rbq, 2)

        def attention(z):
            sum_finish(QKV_B, z, sbq, rbq)
            cos = cos_ref[z]
            sin = sin_ref[z]

            def head(i):
                return total(QKV_B, z, sbq, rbq, slice(i * HD, (i + 1) * HD))

            def rope(v):
                return (v * cos + pltpu.roll(v, HD // 2, 1) * sin).astype(BF16).astype(F32)

            seqs = slice(z * SZ, (z + 1) * SZ)
            for h in range(QH):
                v = rope(head(h))
                for s in range(STEPS):
                    qs[:, s * 8 + h, :] = v[s * SZ:(s + 1) * SZ]
            for h in range(KH):
                v = rope(head(QH + h))
                w = head(QH + KH + h)
                for s in range(STEPS):
                    kn_ref[l, seqs, s * KH + h, :] = v[s * SZ:(s + 1) * SZ]
                    vn_ref[l, seqs, s * KH + h, :] = w[s * SZ:(s + 1) * SZ]

            qall = qs[...].reshape(rows, HD).astype(BF16)
            knew = kn_ref[l, seqs].reshape(SZ * 8, HD).astype(BF16)
            vnew = vn_ref[l, seqs].reshape(SZ * 8, HD).astype(BF16)
            s_new = lax.dot_general(qall, knew, NT, preferred_element_type=F32) * sc
            sn[...] = jnp.where(new_ok, s_new, -jnp.inf).reshape(SZ, 16, SZ * 8)
            if z == 0:
                wwait(l, 3, 4)
            kvrow = jnp.where(lax.broadcasted_iota(jnp.int32, (16, SLOTS), 0) % 8 >= G, 1, 0)
            kcol = lax.broadcasted_iota(jnp.int32, (16, SLOTS), 1)
            parity = (kcol % KH) == kvrow

            def attend(b, carry):
                q = z * SZ + b
                s = lax.dot_general(qs[b].astype(BF16), ck[l, q], NT, preferred_element_type=F32) * sc
                s = jnp.where(parity & (kcol < len_ref[q] * KH), s, -jnp.inf)
                t = sn[b]
                m = jnp.maximum(jnp.max(s, axis=-1, keepdims=True), jnp.max(t, axis=-1, keepdims=True))
                e = jnp.exp(s - m)
                f = jnp.exp(t - m)
                den = jnp.sum(e, axis=-1, keepdims=True) + jnp.sum(f, axis=-1, keepdims=True)
                pn[b] = (f / den).astype(BF16)
                os[b] = jnp.dot((e / den).astype(BF16), cv[l, q], preferred_element_type=F32)
                return carry

            lax.fori_loop(0, SZ, attend, 0, unroll=4)
            o_new = jnp.dot(pn[...].reshape(rows, SZ * 8), vnew, preferred_element_type=F32)
            os[...] = os[...] + o_new.reshape(SZ, 16, HD)
            for h in range(QH):
                o = jnp.concatenate([os[:, s * 8 + h, :] for s in range(STEPS)], axis=0)
                ago[z, own + h // per, :, (h % per) * HD:(h % per + 1) * HD] = o.astype(BF16)
            start(gather(O_COL, z, ago))

        def o_row(z):
            finish(gather(O_COL, z, ago))
            spread_start(O_ROW, z, ago, no)

        def project(act, z, w, depth, ph):
            lhs = act[z].reshape(ALL, depth)
            for h in range(HALVES):
                put(sbo, z, slice(h * WB, (h + 1) * WB),
                    jnp.dot(lhs, w[l, :, h * WB:(h + 1) * WB], preferred_element_type=F32))
            sum_start(ph, z, sbo, pro, rbo)

        def out(z):
            finish(spread(O_ROW, z, ago, no))
            if z == 0:
                wwait(l, 5)
            project(no, z, wo, WB, OUT_B)

        def residual(z, ph, ph_col):
            sum_finish(ph, z, sbo, rbo)
            for h in range(HALVES):
                a = total(ph, z, sbo, rbo, slice(h * WB, (h + 1) * WB))
                x[z, own + h] = (x[z, own + h].astype(F32) + a).astype(BF16)
            start(gather(ph_col, z, x))

        def mlp_norm(z):
            finish(gather(X_MID, z, x))
            norm(z, L + l, None)
            spread_start(N_MLP, z, ns, nb)

        def gate_up(z):
            finish(spread(N_MLP, z, ns, nb))
            if z == 0:
                wwait(l, 6, 7)

            def body(t, carry):
                off = pl.multiple_of(t * tile, tile)
                n = nb[z].reshape(ALL, WB)
                for k, w in enumerate((wg, wu)):
                    put(sbg, z, pl.ds(off + k * FF, tile), jnp.dot(n, w[l, :, pl.ds(off, tile)], preferred_element_type=F32))
                return carry

            lax.fori_loop(0, 4, body, 0)
            sum_start(GU_B, z, sbg, prg, rbg)

        def gate_up_middle(z):
            sum_middle(GU_B, z, sbg, prg, rbg, 8)

        def act(z):
            sum_finish(GU_B, z, sbg, rbg)
            per_half = half // tile

            def body(t, carry):
                off = pl.multiple_of(t * tile, tile)
                g = total(GU_B, z, sbg, rbg, pl.ds(off, tile))
                u = total(GU_B, z, sbg, rbg, pl.ds(off + FF, tile))
                aga[z, own + t // per_half, :, pl.ds(pl.multiple_of((t % per_half) * tile, tile), tile)] = (jax.nn.silu(g) * u).astype(BF16)
                return carry

            lax.fori_loop(0, 4, body, 0)
            start(gather(A_COL, z, aga))

        def a_row(z):
            finish(gather(A_COL, z, aga))
            spread_start(A_ROW, z, aga, na)

        def down(z):
            finish(spread(A_ROW, z, aga, na))
            if z == 0:
                wwait(l, 8)
            project(na, z, wd, half, DOWN_B)

        def end_norm(z):
            finish(gather(X_END, z, x))
            norm(z, l + 1, l == L - 1)
            spread_start(N_ATTN, z, ns, nb)

        stages = [qkv, qkv_middle, attention, o_row, out]
        stages += [lambda z: sum_middle(OUT_B, z, sbo, pro, rbo, 1)] if PRE[OUT_B] is not None else []
        stages += [lambda z: residual(z, OUT_B, X_MID), mlp_norm, gate_up, gate_up_middle, act, a_row, down]
        stages += [lambda z: sum_middle(DOWN_B, z, sbo, pro, rbo, 1)] if PRE[DOWN_B] is not None else []
        stages += [lambda z: residual(z, DOWN_B, X_END), end_norm]
        for stage in stages:
            for z in range(STREAMS):
                stage(z)
        return carry

    lax.fori_loop(0, L, layer_body, 0)
    for z in range(STREAMS):
        finish(spread(N_ATTN, z, ns, nb))
    for b in range(R):
        v = [nb[z, b].astype(F32) for z in range(STREAMS)]
        for s, out in enumerate((out0, out1)):
            out[b * SEQ:(b + 1) * SEQ] = jnp.concatenate([w[s * SZ:(s + 1) * SZ] for w in v], axis=0).astype(BF16)


def cache_kernel(heads, len_ref, kn_h, vn_h, ck_ref, cv_ref, a0, a1, ok_ref, ov_ref, o0, o1,
                 kn_ref, vn_ref, kbuf, vbuf, b0, b1, rsem, wsem, nsem):
    layers, seqs, rows, width = ck_ref.shape
    group = seqs // COPY_GROUPS
    sides = ((ck_ref, kbuf, kn_ref, ok_ref), (cv_ref, vbuf, vn_ref, ov_ref))
    small = [pltpu.make_async_copy(a, b, nsem.at[i]) for i, (a, b) in enumerate(((kn_h, kn_ref), (vn_h, vn_ref), (a0, b0), (a1, b1)))]
    pass_on = [pltpu.make_async_copy(a, b, nsem.at[4 + i]) for i, (a, b) in enumerate(((b0, o0), (b1, o1)))]

    def load(k, i):
        at = (i // COPY_GROUPS, pl.ds((i % COPY_GROUPS) * group, group))
        return pltpu.make_async_copy(sides[k][0].at[at], sides[k][1].at[i], rsem.at[k, i])

    def save(k, i):
        at = (i // COPY_GROUPS, pl.ds((i % COPY_GROUPS) * group, group))
        return pltpu.make_async_copy(sides[k][1].at[i], sides[k][3].at[at], wsem.at[k, i])

    count = layers * COPY_GROUPS
    for cp in small:
        cp.start()
    for i in range(count):
        for k in range(2):
            load(k, i).start()
    for cp in small:
        cp.wait()
    for cp in pass_on:
        cp.start()
    for i in range(count):
        layer, first = i // COPY_GROUPS, (i % COPY_GROUPS) * group
        for k in range(2):
            load(k, i).wait()

            def patch(g, carry):
                buf, fresh = sides[k][1], sides[k][2]
                at = len_ref[first + g] * heads
                base = pl.multiple_of(jnp.minimum((at // 16) * 16, rows - 32), 16)
                win = pl.ds(base, 32)
                idx = lax.broadcasted_iota(jnp.int32, (32, width), 0) + base - at
                val = buf[i, g, win, :].astype(F32)
                new = fresh[layer, first + g]
                for n in range(STEPS * heads):
                    val = jnp.where(idx == n, new[n:n + 1, :], val)
                buf[i, g, win, :] = val.astype(BF16)
                return carry

            lax.fori_loop(0, group, patch, 0, unroll=True)
            save(k, i).start()
    for cp in pass_on:
        cp.wait()
    for i in range(count):
        for k in range(2):
            save(k, i).wait()


def solution(mesh):
    R, C = mesh.shape['row'], mesh.shape['col']
    hidden_spec = P('rep', 'row')
    index_spec = P(('rep', 'row'))
    cache_spec = P(None, ('rep', 'row'), None, 'col', None)
    gain_spec = P(None, 'row')
    weight_spec = P(None, 'row', 'col')

    def device_program(hidden_0, hidden_1, positions, lengths, cache_k, cache_v, norm_attn, norm_mlp, w_query, w_key, w_value, w_out, w_gate, w_up, w_down):
        L, SEQ, CTX, KH, HD = cache_k.shape
        WB = hidden_0.shape[1]
        SZ = SEQ // STREAMS
        TOK = SZ * STEPS
        XS = R // CORES
        Z = STREAMS
        QC, KC, FF = w_query.shape[-1], w_key.shape[-1], w_gate.shape[-1]
        HALVES = R // C
        SLOTS = CTX * KH
        ck = cache_k.reshape(L, SEQ, SLOTS, HD)
        cv = cache_v.reshape(L, SEQ, SLOTS, HD)
        vm = pl.BlockSpec(memory_space=pltpu.VMEM)
        smem = pl.BlockSpec(memory_space=pltpu.SMEM)
        hbm = pl.BlockSpec(memory_space=pl.ANY)
        weights = (w_query, w_key, w_value, w_out, w_gate, w_up, w_down)
        scratch = [pltpu.VMEM(w.shape, BF16) for w in weights] + [pltpu.VMEM(ck.shape, BF16)] * 2
        N3 = QC + 2 * KC
        N2 = 2 * FF
        OUTW = HALVES * WB

        def slots(ph):
            return R - 1 if PRE[ph] is None else XS - 1

        scratch += [pltpu.VMEM(s, d) for s, d in (
            ((Z, TOK, HD), F32), ((Z, TOK, HD), F32), ((8, WB), F32),
            ((Z, R, TOK, WB), BF16), ((Z, R, TOK, WB), BF16), ((R, 8, WB), F32), ((Z, R, TOK, WB), BF16), ((Z, R, TOK, WB), BF16),
            ((Z, CORES, XS, TOK, N3), BF16), ((Z, XS, TOK, N3), BF16), ((Z, slots(QKV_B), TOK, N3), BF16),
            ((SZ, 16, HD), F32), ((SZ, 16, SZ * 8), F32), ((SZ, 16, SZ * 8), BF16), ((SZ, 16, HD), F32),
            ((Z, R, TOK, WB), BF16), ((Z, R, TOK, WB), BF16),
            ((Z, CORES, XS, TOK, OUTW), BF16), ((Z, XS, TOK, OUTW), BF16), ((Z, slots(OUT_B), TOK, OUTW), BF16),
            ((Z, CORES, XS, TOK, N2), BF16), ((Z, XS, TOK, N2), BF16), ((Z, slots(GU_B), TOK, N2), BF16),
            ((Z, R, TOK, FF // HALVES), BF16), ((Z, R, TOK, FF // HALVES), BF16))]
        scratch += [pltpu.SemaphoreType.DMA((PHASES, Z, R - 1))] * 2 + [pltpu.SemaphoreType.DMA((L, 9))]
        dims = dict(R=R, C=C, L=L, D=WB * R, HD=HD)
        out_0, out_1, k_new, v_new = pl.pallas_call(
            functools.partial(decode_kernel, dims),
            out_shape=(jax.ShapeDtypeStruct(hidden_0.shape, BF16), jax.ShapeDtypeStruct(hidden_1.shape, BF16),
                       jax.ShapeDtypeStruct((L, SEQ, 8, HD), F32), jax.ShapeDtypeStruct((L, SEQ, 8, HD), F32)),
            in_specs=[vm, vm, smem, smem, vm, vm] + [hbm] * 9,
            out_specs=(vm, vm, vm, vm),
            scratch_shapes=scratch,
            compiler_params=pltpu.CompilerParams(collective_id=0, has_side_effects=True, vmem_limit_bytes=62 * 1024 * 1024),
            name='decode',
        )(hidden_0, hidden_1, positions, lengths, norm_attn, norm_mlp, *weights, ck, cv)

        count = L * COPY_GROUPS
        buf = pltpu.VMEM((count, SEQ // COPY_GROUPS, SLOTS, HD), BF16)
        fresh = pltpu.VMEM(k_new.shape, F32)
        hidden = pltpu.VMEM(hidden_0.shape, BF16)
        ok, ov, out_0, out_1 = pl.pallas_call(
            functools.partial(cache_kernel, KH),
            out_shape=(jax.ShapeDtypeStruct(ck.shape, BF16),) * 2 + (jax.ShapeDtypeStruct(hidden_0.shape, BF16),) * 2,
            in_specs=[smem] + [hbm] * 6,
            out_specs=(hbm,) * 4,
            scratch_shapes=[fresh, fresh, buf, buf, hidden, hidden, pltpu.SemaphoreType.DMA((2, count)),
                            pltpu.SemaphoreType.DMA((2, count)), pltpu.SemaphoreType.DMA((6,))],
            compiler_params=pltpu.CompilerParams(vmem_limit_bytes=62 * 1024 * 1024),
            name='cache_update',
        )(lengths, k_new, v_new, ck, cv, out_0, out_1)
        ok, ov = ok.reshape(cache_k.shape), ov.reshape(cache_v.shape)
        return out_0, out_1, ok, ov

    return jax.shard_map(device_program, mesh=mesh,
                         in_specs=(hidden_spec, hidden_spec, index_spec, index_spec, cache_spec, cache_spec, gain_spec, gain_spec) + (weight_spec,) * 7,
                         out_specs=(hidden_spec, hidden_spec, cache_spec, cache_spec), check_vma=False)
```

```python
import functools
import math

import jax
import jax.numpy as jnp
from jax import lax
from jax.experimental import pallas as pl
from jax.experimental.pallas import tpu as pltpu
from jax.sharding import PartitionSpec as P

ROPE_BASE = 1000000.0
EPS = 1e-05
F32 = jnp.float32
BF16 = jnp.bfloat16
STEPS = 2
MESH = pl.DeviceIdType.MESH
NT = (((1,), (1,)), ((), ()))

CORES = 2
COPY_GROUPS = 4
STREAMS = 4

(X_INIT, GAIN, N_ATTN, QKV_A, QKV_B, O_COL, O_ROW, OUT_A, OUT_B, X_MID, N_MLP, GU_A, GU_B, A_COL, A_ROW, DOWN_A, DOWN_B,
 X_END, PHASES) = range(19)
PRE = {QKV_B: None, GU_B: GU_A, OUT_B: None, DOWN_B: None}


def decode_kernel(dims, h0, h1, pos_ref, len_ref, ga_ref, gm_ref, wq_h, wk_h, wv_h, wo_h, wg_h, wu_h, wd_h, ck_h, cv_h,
                  out0, out1, kn_ref, vn_ref,
                  wq, wk, wv, wo, wg, wu, wd, ck, cv,
                  cos_ref, sin_ref, gain_ref, xb, x, gains, ns, nb, sbq, prq, rbq, qs, sn, pn, os, ago, no, sbo, pro, rbo, sbg, prg, rbg, aga, na,
                  ssem, rsem, wsem):
    R, C, L, D = dims['R'], dims['C'], dims['L'], dims['D']
    HD = dims['HD']
    SEQ = h0.shape[0] // R
    SZ = SEQ // STREAMS
    TOK = SZ * STEPS
    ALL = TOK * R
    WB = h0.shape[1]
    QC, KC = wq.shape[-1], wk.shape[-1]
    QH, KH = QC // HD, KC // HD
    G = QH // KH
    FF = wg.shape[-1]
    HALVES = R // C
    SLOTS = ck.shape[2]
    XS = R // CORES
    r = lax.axis_index('row')
    c = lax.axis_index('col')
    chip, core = lax.div(r, CORES), lax.rem(r, CORES)
    own = c * HALVES
    mine = pl.ds(own, HALVES)

    pairs = [(wq_h, wq), (wk_h, wk), (wv_h, wv), (ck_h, ck), (cv_h, cv), (wo_h, wo), (wg_h, wg), (wu_h, wu), (wd_h, wd)]

    def fetch(layer, i):
        return pltpu.make_async_copy(pairs[i][0].at[layer], pairs[i][1].at[layer], wsem.at[layer, i])

    def wwait(layer, *which):
        for i in which:
            fetch(layer, i).wait()

    for i in range(len(pairs)):
        fetch(0, i).start()

    barrier = pltpu.get_barrier_semaphore()
    for j in range(1, R):
        pl.semaphore_signal(barrier, inc=1, device_id={'row': lax.rem(r + j, R)}, device_id_type=MESH)
    for j in range(1, C):
        pl.semaphore_signal(barrier, inc=1, device_id={'col': lax.rem(c + j, C)}, device_id_type=MESH)

    def remote(ph, z, src, dst, device):
        pltpu.make_async_remote_copy(src_ref=src, dst_ref=dst, send_sem=ssem.at[ph, z], recv_sem=rsem.at[ph, z],
                                     device_id=device, device_id_type=MESH).start()

    def finish(ph, z, received):
        pltpu.make_async_copy(received, received, rsem.at[ph, z]).wait()
        pltpu.make_async_copy(received, received, ssem.at[ph, z]).wait()

    def row_send(ph, z, src, dst):
        for j in range(1, R):
            peer = lax.rem(r + j, R)
            remote(ph, z, src(peer), dst(j), {'row': peer})

    def spread_start(ph, z, src, dst):
        row_send(ph, z, lambda peer: src.at[z, peer], lambda j: dst.at[z, r])
        dst[z, r] = src[z, r]

    def spread_finish(ph, z, dst):
        finish(ph, z, dst.at[z, pl.ds(0, R - 1)])

    def gather_start(ph, z, buf):
        for j in range(1, C):
            remote(ph, z, buf.at[z, mine], buf.at[z, mine], {'col': lax.rem(c + j, C)})

    def gather_finish(ph, z, buf):
        finish(ph, z, buf.at[z, pl.ds(0, (C - 1) * HALVES)])

    def sum_start(ph, z, sb, pr, rb):
        if PRE[ph] is not None:
            remote(PRE[ph], z, sb.at[z, 1 - core], pr.at[z], {'row': r + 1 - 2 * core})
        else:
            row_send(ph, z, lambda peer: sb.at[z, lax.rem(peer, CORES), lax.div(peer, CORES)], lambda j: rb.at[z, j - 1])

    def sum_middle(ph, z, sb, pr, rb, tiles):
        if PRE[ph] is None:
            return
        finish(PRE[ph], z, pr.at[z])
        width = sb.shape[-1] // tiles

        def add(t, carry):
            sl = pl.ds(pl.multiple_of(t * width, width), width)
            sb[z, core, :, :, sl] = (sb[z, core, :, :, sl].astype(F32) + pr[z, :, :, sl].astype(F32)).astype(BF16)
            return carry

        lax.fori_loop(0, tiles, add, 0)
        for j in range(1, XS):
            peer = lax.rem(chip + j, XS)
            remote(ph, z, sb.at[z, core, peer], rb.at[z, j - 1], {'row': peer * CORES + core})

    def sum_finish(ph, z, sb, rb):
        finish(ph, z, rb.at[z])

    def total(ph, z, sb, rb, sl):
        a = sb[z, core, chip, :, sl].astype(F32)
        for j in range((XS if PRE[ph] is not None else R) - 1):
            a = a + rb[z, j, :, sl].astype(F32)
        return a.astype(BF16).astype(F32)

    def put(sb, z, cols, res):
        v = res.astype(BF16).reshape(XS, CORES, TOK, res.shape[-1])
        for k in range(CORES):
            sb[z, k, :, :, cols] = v[:, k]

    def norm(z, gi, last):
        ss = jnp.zeros((TOK, 1), F32)
        for k in range(R):
            xk = x[z, k].astype(F32)
            ss = ss + jnp.sum(xk * xk, axis=-1, keepdims=True)
        scale = lax.rsqrt(ss / D + EPS)
        for k in range(R):
            xk = x[z, k].astype(F32)
            n = xk * scale * gains[k, pl.ds(gi, 1), :]
            if last is not None:
                n = jnp.where(last, xk, n)
            ns[z, k] = n.astype(BF16)

    gain_ref[...] = jnp.zeros_like(gain_ref)
    gain_ref[0:L] = ga_ref[...].astype(F32)
    gain_ref[L:2 * L] = gm_ref[...].astype(F32)
    lane = lax.broadcasted_iota(jnp.int32, (TOK, HD), 1)
    token = lax.broadcasted_iota(jnp.int32, (TOK, HD), 0)
    half_lane = lax.rem(lane, HD // 2)
    inv_freq = jnp.exp(half_lane.astype(F32) * (-2.0 / HD * math.log(ROPE_BASE)))
    for z in range(STREAMS):
        position = jnp.zeros((TOK, HD), jnp.int32)
        for b in range(SZ):
            position = jnp.where(lax.rem(token, SZ) == b, pos_ref[z * SZ + b], position)
        angle = (position + lax.div(token, SZ)).astype(F32) * inv_freq
        cos_ref[z] = jnp.cos(angle)
        sine = jnp.sin(angle)
        sin_ref[z] = jnp.where(lane < HD // 2, -sine, sine)

    for b in range(R):
        v0 = h0[b * SEQ:(b + 1) * SEQ].astype(F32)
        v1 = h1[b * SEQ:(b + 1) * SEQ].astype(F32)
        for z in range(STREAMS):
            part = slice(z * SZ, (z + 1) * SZ)
            xb[z, b] = jnp.concatenate([v0[part], v1[part]], axis=0).astype(BF16)
    qs[...] = jnp.zeros_like(qs)
    kn_ref[...] = jnp.zeros_like(kn_ref)
    vn_ref[...] = jnp.zeros_like(vn_ref)
    pl.semaphore_wait(barrier, R + C - 2)

    for z in range(STREAMS):
        spread_start(X_INIT, z, xb, x)
        if z == 0:
            row_send(GAIN, 0, lambda peer: gain_ref, lambda j: gains.at[r])
    gains[r] = gain_ref[...]
    for layer in range(1, L):
        for i in range(len(pairs)):
            fetch(layer, i).start()
    for z in range(STREAMS):
        spread_finish(X_INIT, z, x)
        if z == 0:
            finish(GAIN, 0, gains.at[pl.ds(0, R - 1)])
        norm(z, 0, None)
        spread_start(N_ATTN, z, ns, nb)

    rows = SZ * 16
    sc = HD ** -0.5
    ri = lax.broadcasted_iota(jnp.int32, (rows, SZ * 8), 0)
    ci = lax.broadcasted_iota(jnp.int32, (rows, SZ * 8), 1)
    slot = ci % 8
    kvh = jnp.where(ri % 8 >= G, 1, 0)
    new_ok = (ri // 16 == ci // 8) & (slot < STEPS * KH) & (slot % KH == kvh) & (slot // KH <= (ri % 16) // 8)
    per = QH // HALVES
    tile = FF // 4
    half = FF // HALVES

    def layer_body(l, carry):
        def qkv(z):
            spread_finish(N_ATTN, z, nb)
            if z == 0:
                wwait(l, 0, 1, 2)
            n = nb[z].reshape(ALL, WB)
            col = 0
            for w, width in ((wq, QC), (wk, KC), (wv, KC)):
                put(sbq, z, slice(col, col + width), jnp.dot(n, w[l], preferred_element_type=F32))
                col += width
            sum_start(QKV_B, z, sbq, prq, rbq)

        def qkv_middle(z):
            sum_middle(QKV_B, z, sbq, prq, rbq, 2)

        def attention(z):
            sum_finish(QKV_B, z, sbq, rbq)
            cos = cos_ref[z]
            sin = sin_ref[z]

            def head(i):
                return total(QKV_B, z, sbq, rbq, slice(i * HD, (i + 1) * HD))

            def rope(v):
                return (v * cos + pltpu.roll(v, HD // 2, 1) * sin).astype(BF16).astype(F32)

            seqs = slice(z * SZ, (z + 1) * SZ)
            for h in range(QH):
                v = rope(head(h))
                for s in range(STEPS):
                    qs[:, s * 8 + h, :] = v[s * SZ:(s + 1) * SZ]
            for h in range(KH):
                v = rope(head(QH + h))
                w = head(QH + KH + h)
                for s in range(STEPS):
                    kn_ref[l, seqs, s * KH + h, :] = v[s * SZ:(s + 1) * SZ]
                    vn_ref[l, seqs, s * KH + h, :] = w[s * SZ:(s + 1) * SZ]

            qall = qs[...].reshape(rows, HD).astype(BF16)
            knew = kn_ref[l, seqs].reshape(SZ * 8, HD).astype(BF16)
            vnew = vn_ref[l, seqs].reshape(SZ * 8, HD).astype(BF16)
            s_new = lax.dot_general(qall, knew, NT, preferred_element_type=F32) * sc
            sn[...] = jnp.where(new_ok, s_new, -jnp.inf).reshape(SZ, 16, SZ * 8)
            if z == 0:
                wwait(l, 3, 4)
            kvrow = jnp.where(lax.broadcasted_iota(jnp.int32, (16, SLOTS), 0) % 8 >= G, 1, 0)
            kcol = lax.broadcasted_iota(jnp.int32, (16, SLOTS), 1)
            parity = (kcol % KH) == kvrow

            def attend(b, carry):
                q = z * SZ + b
                s = lax.dot_general(qs[b].astype(BF16), ck[l, q], NT, preferred_element_type=F32) * sc
                s = jnp.where(parity & (kcol < len_ref[q] * KH), s, -jnp.inf)
                t = sn[b]
                m = jnp.maximum(jnp.max(s, axis=-1, keepdims=True), jnp.max(t, axis=-1, keepdims=True))
                e = jnp.exp(s - m)
                f = jnp.exp(t - m)
                den = jnp.sum(e, axis=-1, keepdims=True) + jnp.sum(f, axis=-1, keepdims=True)
                pn[b] = (f / den).astype(BF16)
                os[b] = jnp.dot((e / den).astype(BF16), cv[l, q], preferred_element_type=F32)
                return carry

            lax.fori_loop(0, SZ, attend, 0, unroll=4)
            o_new = jnp.dot(pn[...].reshape(rows, SZ * 8), vnew, preferred_element_type=F32)
            os[...] = os[...] + o_new.reshape(SZ, 16, HD)
            for h in range(QH):
                o = jnp.concatenate([os[:, s * 8 + h, :] for s in range(STEPS)], axis=0)
                ago[z, own + h // per, :, (h % per) * HD:(h % per + 1) * HD] = o.astype(BF16)
            gather_start(O_COL, z, ago)

        def o_row(z):
            gather_finish(O_COL, z, ago)
            spread_start(O_ROW, z, ago, no)

        def project(act, z, w, depth, ph):
            lhs = act[z].reshape(ALL, depth)
            for h in range(HALVES):
                put(sbo, z, slice(h * WB, (h + 1) * WB),
                    jnp.dot(lhs, w[l, :, h * WB:(h + 1) * WB], preferred_element_type=F32))
            sum_start(ph, z, sbo, pro, rbo)

        def out(z):
            spread_finish(O_ROW, z, no)
            if z == 0:
                wwait(l, 5)
            project(no, z, wo, WB, OUT_B)

        def residual(z, ph, ph_col):
            sum_finish(ph, z, sbo, rbo)
            for h in range(HALVES):
                a = total(ph, z, sbo, rbo, slice(h * WB, (h + 1) * WB))
                x[z, own + h] = (x[z, own + h].astype(F32) + a).astype(BF16)
            gather_start(ph_col, z, x)

        def mlp_norm(z):
            gather_finish(X_MID, z, x)
            norm(z, L + l, None)
            spread_start(N_MLP, z, ns, nb)

        def gate_up(z):
            spread_finish(N_MLP, z, nb)
            if z == 0:
                wwait(l, 6, 7)

            def body(t, carry):
                off = pl.multiple_of(t * tile, tile)
                n = nb[z].reshape(ALL, WB)
                for k, w in enumerate((wg, wu)):
                    put(sbg, z, pl.ds(off + k * FF, tile), jnp.dot(n, w[l, :, pl.ds(off, tile)], preferred_element_type=F32))
                return carry

            lax.fori_loop(0, 4, body, 0)
            sum_start(GU_B, z, sbg, prg, rbg)

        def gate_up_middle(z):
            sum_middle(GU_B, z, sbg, prg, rbg, 8)

        def act(z):
            sum_finish(GU_B, z, sbg, rbg)
            per_half = half // tile

            def body(t, carry):
                off = pl.multiple_of(t * tile, tile)
                g = total(GU_B, z, sbg, rbg, pl.ds(off, tile))
                u = total(GU_B, z, sbg, rbg, pl.ds(off + FF, tile))
                aga[z, own + t // per_half, :, pl.ds(pl.multiple_of((t % per_half) * tile, tile), tile)] = (jax.nn.silu(g) * u).astype(BF16)
                return carry

            lax.fori_loop(0, 4, body, 0)
            gather_start(A_COL, z, aga)

        def a_row(z):
            gather_finish(A_COL, z, aga)
            spread_start(A_ROW, z, aga, na)

        def down(z):
            spread_finish(A_ROW, z, na)
            if z == 0:
                wwait(l, 8)
            project(na, z, wd, half, DOWN_B)

        def end_norm(z):
            gather_finish(X_END, z, x)
            norm(z, l + 1, l == L - 1)
            spread_start(N_ATTN, z, ns, nb)

        stages = [qkv, qkv_middle, attention, o_row, out]
        stages += [lambda z: sum_middle(OUT_B, z, sbo, pro, rbo, 1)] if PRE[OUT_B] is not None else []
        stages += [lambda z: residual(z, OUT_B, X_MID), mlp_norm, gate_up, gate_up_middle, act, a_row, down]
        stages += [lambda z: sum_middle(DOWN_B, z, sbo, pro, rbo, 1)] if PRE[DOWN_B] is not None else []
        stages += [lambda z: residual(z, DOWN_B, X_END), end_norm]
        for stage in stages:
            for z in range(STREAMS):
                stage(z)
        return carry

    lax.fori_loop(0, L, layer_body, 0)
    for z in range(STREAMS):
        spread_finish(N_ATTN, z, nb)
    for b in range(R):
        v = [nb[z, b].astype(F32) for z in range(STREAMS)]
        for s, out in enumerate((out0, out1)):
            out[b * SEQ:(b + 1) * SEQ] = jnp.concatenate([w[s * SZ:(s + 1) * SZ] for w in v], axis=0).astype(BF16)


def cache_kernel(heads, len_ref, kn_h, vn_h, ck_ref, cv_ref, a0, a1, ok_ref, ov_ref, o0, o1,
                 kn_ref, vn_ref, kbuf, vbuf, b0, b1, rsem, wsem, nsem):
    layers, seqs, rows, width = ck_ref.shape
    group = seqs // COPY_GROUPS
    sides = ((ck_ref, kbuf, kn_ref, ok_ref), (cv_ref, vbuf, vn_ref, ov_ref))
    small = [pltpu.make_async_copy(a, b, nsem.at[i]) for i, (a, b) in enumerate(((kn_h, kn_ref), (vn_h, vn_ref), (a0, b0), (a1, b1)))]
    pass_on = [pltpu.make_async_copy(a, b, nsem.at[4 + i]) for i, (a, b) in enumerate(((b0, o0), (b1, o1)))]

    def load(k, i):
        at = (i // COPY_GROUPS, pl.ds((i % COPY_GROUPS) * group, group))
        return pltpu.make_async_copy(sides[k][0].at[at], sides[k][1].at[i], rsem.at[k, i])

    def save(k, i):
        at = (i // COPY_GROUPS, pl.ds((i % COPY_GROUPS) * group, group))
        return pltpu.make_async_copy(sides[k][1].at[i], sides[k][3].at[at], wsem.at[k, i])

    count = layers * COPY_GROUPS
    for cp in small:
        cp.start()
    for i in range(count):
        for k in range(2):
            load(k, i).start()
    for cp in small:
        cp.wait()
    for cp in pass_on:
        cp.start()
    for i in range(count):
        layer, first = i // COPY_GROUPS, (i % COPY_GROUPS) * group
        for k in range(2):
            load(k, i).wait()

            def patch(g, carry):
                buf, fresh = sides[k][1], sides[k][2]
                at = len_ref[first + g] * heads
                base = pl.multiple_of(jnp.minimum((at // 16) * 16, rows - 32), 16)
                win = pl.ds(base, 32)
                idx = lax.broadcasted_iota(jnp.int32, (32, width), 0) + base - at
                val = buf[i, g, win, :].astype(F32)
                new = fresh[layer, first + g]
                for n in range(STEPS * heads):
                    val = jnp.where(idx == n, new[n:n + 1, :], val)
                buf[i, g, win, :] = val.astype(BF16)
                return carry

            lax.fori_loop(0, group, patch, 0, unroll=True)
            save(k, i).start()
    for cp in pass_on:
        cp.wait()
    for i in range(count):
        for k in range(2):
            save(k, i).wait()


def solution(mesh):
    R, C = mesh.shape['row'], mesh.shape['col']
    hidden_spec = P('rep', 'row')
    index_spec = P(('rep', 'row'))
    cache_spec = P(None, ('rep', 'row'), None, 'col', None)
    gain_spec = P(None, 'row')
    weight_spec = P(None, 'row', 'col')

    def device_program(hidden_0, hidden_1, positions, lengths, cache_k, cache_v, norm_attn, norm_mlp, w_query, w_key, w_value, w_out, w_gate, w_up, w_down):
        L, SEQ, CTX, KH, HD = cache_k.shape
        WB = hidden_0.shape[1]
        SZ = SEQ // STREAMS
        TOK = SZ * STEPS
        XS = R // CORES
        Z = STREAMS
        QC, KC, FF = w_query.shape[-1], w_key.shape[-1], w_gate.shape[-1]
        HALVES = R // C
        SLOTS = CTX * KH
        ck = cache_k.reshape(L, SEQ, SLOTS, HD)
        cv = cache_v.reshape(L, SEQ, SLOTS, HD)
        vm = pl.BlockSpec(memory_space=pltpu.VMEM)
        smem = pl.BlockSpec(memory_space=pltpu.SMEM)
        hbm = pl.BlockSpec(memory_space=pl.ANY)
        weights = (w_query, w_key, w_value, w_out, w_gate, w_up, w_down)
        scratch = [pltpu.VMEM(w.shape, BF16) for w in weights] + [pltpu.VMEM(ck.shape, BF16)] * 2
        N3 = QC + 2 * KC
        N2 = 2 * FF
        OUTW = HALVES * WB

        def slots(ph):
            return R - 1 if PRE[ph] is None else XS - 1

        scratch += [pltpu.VMEM(s, d) for s, d in (
            ((Z, TOK, HD), F32), ((Z, TOK, HD), F32), ((8, WB), F32),
            ((Z, R, TOK, WB), BF16), ((Z, R, TOK, WB), BF16), ((R, 8, WB), F32), ((Z, R, TOK, WB), BF16), ((Z, R, TOK, WB), BF16),
            ((Z, CORES, XS, TOK, N3), BF16), ((Z, XS, TOK, N3), BF16), ((Z, slots(QKV_B), TOK, N3), BF16),
            ((SZ, 16, HD), F32), ((SZ, 16, SZ * 8), F32), ((SZ, 16, SZ * 8), BF16), ((SZ, 16, HD), F32),
            ((Z, R, TOK, WB), BF16), ((Z, R, TOK, WB), BF16),
            ((Z, CORES, XS, TOK, OUTW), BF16), ((Z, XS, TOK, OUTW), BF16), ((Z, slots(OUT_B), TOK, OUTW), BF16),
            ((Z, CORES, XS, TOK, N2), BF16), ((Z, XS, TOK, N2), BF16), ((Z, slots(GU_B), TOK, N2), BF16),
            ((Z, R, TOK, FF // HALVES), BF16), ((Z, R, TOK, FF // HALVES), BF16))]
        scratch += [pltpu.SemaphoreType.DMA((PHASES, Z))] * 2 + [pltpu.SemaphoreType.DMA((L, 9))]
        dims = dict(R=R, C=C, L=L, D=WB * R, HD=HD)
        out_0, out_1, k_new, v_new = pl.pallas_call(
            functools.partial(decode_kernel, dims),
            out_shape=(jax.ShapeDtypeStruct(hidden_0.shape, BF16), jax.ShapeDtypeStruct(hidden_1.shape, BF16),
                       jax.ShapeDtypeStruct((L, SEQ, 8, HD), F32), jax.ShapeDtypeStruct((L, SEQ, 8, HD), F32)),
            in_specs=[vm, vm, smem, smem, vm, vm] + [hbm] * 9,
            out_specs=(vm, vm, vm, vm),
            scratch_shapes=scratch,
            compiler_params=pltpu.CompilerParams(collective_id=0, has_side_effects=True, vmem_limit_bytes=62 * 1024 * 1024),
            name='decode',
        )(hidden_0, hidden_1, positions, lengths, norm_attn, norm_mlp, *weights, ck, cv)

        count = L * COPY_GROUPS
        buf = pltpu.VMEM((count, SEQ // COPY_GROUPS, SLOTS, HD), BF16)
        fresh = pltpu.VMEM(k_new.shape, F32)
        hidden = pltpu.VMEM(hidden_0.shape, BF16)
        ok, ov, out_0, out_1 = pl.pallas_call(
            functools.partial(cache_kernel, KH),
            out_shape=(jax.ShapeDtypeStruct(ck.shape, BF16),) * 2 + (jax.ShapeDtypeStruct(hidden_0.shape, BF16),) * 2,
            in_specs=[smem] + [hbm] * 6,
            out_specs=(hbm,) * 4,
            scratch_shapes=[fresh, fresh, buf, buf, hidden, hidden, pltpu.SemaphoreType.DMA((2, count)),
                            pltpu.SemaphoreType.DMA((2, count)), pltpu.SemaphoreType.DMA((6,))],
            compiler_params=pltpu.CompilerParams(vmem_limit_bytes=62 * 1024 * 1024),
            name='cache_update',
        )(lengths, k_new, v_new, ck, cv, out_0, out_1)
        ok, ov = ok.reshape(cache_k.shape), ov.reshape(cache_v.shape)
        return out_0, out_1, ok, ov

    return jax.shard_map(device_program, mesh=mesh,
                         in_specs=(hidden_spec, hidden_spec, index_spec, index_spec, cache_spec, cache_spec, gain_spec, gain_spec) + (weight_spec,) * 7,
                         out_specs=(hidden_spec, hidden_spec, cache_spec, cache_spec), check_vma=False)
```

```python
import functools
import math

import jax
import jax.numpy as jnp
from jax import lax
from jax.experimental import pallas as pl
from jax.experimental.pallas import tpu as pltpu
from jax.sharding import PartitionSpec as P

ROPE_BASE = 1000000.0
EPS = 1e-05
F32 = jnp.float32
BF16 = jnp.bfloat16
STEPS = 2
MESH = pl.DeviceIdType.MESH
NT = (((1,), (1,)), ((), ()))

CORES = 2
COPY_GROUPS = 4
STREAMS = 4

(X_INIT, SQUARES, GAIN, N_ATTN, QKV_A, QKV_B, O_COL, O_ROW, OUT_A, OUT_B, X_MID, N_MLP, GU_A, GU_B, A_COL, A_ROW, DOWN_A, DOWN_B,
 X_END, PHASES) = range(20)
PRE = {QKV_B: None, GU_B: GU_A, OUT_B: None, DOWN_B: None}


def decode_kernel(dims, h0, h1, pos_ref, len_ref, ga_ref, gm_ref, wq_h, wk_h, wv_h, wo_h, wg_h, wu_h, wd_h, ck_h, cv_h,
                  out0, out1, kn_ref, vn_ref, ck, cv,
                  wq, wk, wv, wo, wg, wu, wd,
                  cos_ref, sin_ref, gain_ref, sq, sqs, xb, x, gains, ns, nb, sbq, prq, rbq, qs, sn, pn, os, ago, no, sbo, pro, rbo, sbg, prg, rbg, aga, na,
                  ssem, rsem, wsem):
    R, C, L, D = dims['R'], dims['C'], dims['L'], dims['D']
    HD = dims['HD']
    SEQ = h0.shape[0] // R
    SZ = SEQ // STREAMS
    TOK = SZ * STEPS
    ALL = TOK * R
    WB = h0.shape[1]
    QC, KC = wq.shape[-1], wk.shape[-1]
    QH, KH = QC // HD, KC // HD
    G = QH // KH
    FF = wg.shape[-1]
    HALVES = R // C
    SLOTS = ck.shape[2]
    XS = R // CORES
    r = lax.axis_index('row')
    c = lax.axis_index('col')
    chip, core = lax.div(r, CORES), lax.rem(r, CORES)
    own = c * HALVES
    mine = pl.ds(own, HALVES)

    pairs = [(wq_h, wq), (wk_h, wk), (wv_h, wv), (ck_h, ck), (cv_h, cv), (wo_h, wo), (wg_h, wg), (wu_h, wu), (wd_h, wd)]

    def fetch(layer, i):
        return pltpu.make_async_copy(pairs[i][0].at[layer], pairs[i][1].at[layer], wsem.at[layer, i])

    def wwait(layer, *which):
        for i in which:
            fetch(layer, i).wait()

    for i in range(len(pairs)):
        fetch(0, i).start()

    barrier = pltpu.get_barrier_semaphore()
    for j in range(1, R):
        pl.semaphore_signal(barrier, inc=1, device_id={'row': lax.rem(r + j, R)}, device_id_type=MESH)
    for j in range(1, C):
        pl.semaphore_signal(barrier, inc=1, device_id={'col': lax.rem(c + j, C)}, device_id_type=MESH)

    def remote(ph, z, src, dst, device):
        pltpu.make_async_remote_copy(src_ref=src, dst_ref=dst, send_sem=ssem.at[ph, z], recv_sem=rsem.at[ph, z],
                                     device_id=device, device_id_type=MESH).start()

    def finish(ph, z, received):
        pltpu.make_async_copy(received, received, rsem.at[ph, z]).wait()
        pltpu.make_async_copy(received, received, ssem.at[ph, z]).wait()

    def row_send(ph, z, src, dst):
        for j in range(1, R):
            peer = lax.rem(r + j, R)
            remote(ph, z, src(peer), dst(j), {'row': peer})

    def spread_start(ph, z, src, dst):
        row_send(ph, z, lambda peer: src.at[z, peer], lambda j: dst.at[z, r])
        dst[z, r] = src[z, r]

    def spread_finish(ph, z, dst):
        finish(ph, z, dst.at[z, pl.ds(0, R - 1)])

    def gather_start(ph, z, buf):
        for j in range(1, C):
            remote(ph, z, buf.at[z, mine], buf.at[z, mine], {'col': lax.rem(c + j, C)})

    def gather_finish(ph, z, buf):
        finish(ph, z, buf.at[z, pl.ds(0, (C - 1) * HALVES)])

    def sum_start(ph, z, sb, pr, rb):
        if PRE[ph] is not None:
            remote(PRE[ph], z, sb.at[z, 1 - core], pr.at[z], {'row': r + 1 - 2 * core})
        else:
            row_send(ph, z, lambda peer: sb.at[z, lax.rem(peer, CORES), lax.div(peer, CORES)], lambda j: rb.at[z, j - 1])

    def sum_middle(ph, z, sb, pr, rb, tiles):
        if PRE[ph] is None:
            return
        finish(PRE[ph], z, pr.at[z])
        width = sb.shape[-1] // tiles

        def add(t, carry):
            sl = pl.ds(pl.multiple_of(t * width, width), width)
            sb[z, core, :, :, sl] = (sb[z, core, :, :, sl].astype(F32) + pr[z, :, :, sl].astype(F32)).astype(BF16)
            return carry

        lax.fori_loop(0, tiles, add, 0)
        for j in range(1, XS):
            peer = lax.rem(chip + j, XS)
            remote(ph, z, sb.at[z, core, peer], rb.at[z, j - 1], {'row': peer * CORES + core})

    def sum_finish(ph, z, sb, rb):
        finish(ph, z, rb.at[z])

    def total(ph, z, sb, rb, sl):
        a = sb[z, core, chip, :, sl].astype(F32)
        for j in range((XS if PRE[ph] is not None else R) - 1):
            a = a + rb[z, j, :, sl].astype(F32)
        return a.astype(BF16).astype(F32)

    def put(sb, z, cols, res):
        v = res.astype(BF16).reshape(XS, CORES, TOK, res.shape[-1])
        for k in range(CORES):
            sb[z, k, :, :, cols] = v[:, k]

    def norm(z, gi, last):
        ss = jnp.zeros((TOK, 1), F32)
        for k in range(R):
            xk = x[z, k].astype(F32)
            ss = ss + jnp.sum(xk * xk, axis=-1, keepdims=True)
        scale = lax.rsqrt(ss / D + EPS)
        for k in range(R):
            xk = x[z, k].astype(F32)
            n = xk if last else xk * scale * gains[k, gi:gi + 1, :]
            ns[z, k] = n.astype(BF16)

    gain_ref[...] = jnp.zeros_like(gain_ref)
    gain_ref[0:L] = ga_ref[...].astype(F32)
    gain_ref[L:2 * L] = gm_ref[...].astype(F32)
    lane = lax.broadcasted_iota(jnp.int32, (TOK, HD), 1)
    token = lax.broadcasted_iota(jnp.int32, (TOK, HD), 0)
    half_lane = lax.rem(lane, HD // 2)
    inv_freq = jnp.exp(half_lane.astype(F32) * (-2.0 / HD * math.log(ROPE_BASE)))
    for z in range(STREAMS):
        position = jnp.zeros((TOK, HD), jnp.int32)
        for b in range(SZ):
            position = jnp.where(lax.rem(token, SZ) == b, pos_ref[z * SZ + b], position)
        angle = (position + lax.div(token, SZ)).astype(F32) * inv_freq
        cos_ref[z] = jnp.cos(angle)
        sine = jnp.sin(angle)
        sin_ref[z] = jnp.where(lane < HD // 2, -sine, sine)

    for b in range(R):
        v0 = h0[b * SEQ:(b + 1) * SEQ].astype(F32)
        v1 = h1[b * SEQ:(b + 1) * SEQ].astype(F32)
        for z in range(STREAMS):
            part = slice(z * SZ, (z + 1) * SZ)
            xb[z, b] = jnp.concatenate([v0[part], v1[part]], axis=0).astype(BF16)
    qs[...] = jnp.zeros_like(qs)
    kn_ref[...] = jnp.zeros_like(kn_ref)
    vn_ref[...] = jnp.zeros_like(vn_ref)
    pl.semaphore_wait(barrier, R + C - 2)

    group = 128 // ALL
    tok = lax.broadcasted_iota(jnp.int32, (ALL, 128), 0)
    spot = lax.broadcasted_iota(jnp.int32, (ALL, 128), 1)
    line = lax.broadcasted_iota(jnp.int32, (8, 128), 0)
    packed = jnp.zeros((8, 128), F32)
    for z in range(STREAMS):
        xz = xb[z].astype(F32).reshape(ALL, WB)
        ss = jnp.sum(xz * xz, axis=-1, keepdims=True)
        lanes = jnp.sum(jnp.where(spot == tok + (z % group) * ALL, ss, 0.0), axis=0, keepdims=True)
        packed = packed + jnp.where(line == z // group, lanes, 0.0)
    sq[...] = packed
    row_send(SQUARES, 0, lambda peer: sq, lambda j: sqs.at[r])
    sqs[r] = sq[...]
    row_send(GAIN, 0, lambda peer: gain_ref, lambda j: gains.at[r])
    gains[r] = gain_ref[...]
    for z in range(STREAMS):
        spread_start(X_INIT, z, xb, x)
    for layer in range(1, L):
        for i in range(len(pairs)):
            fetch(layer, i).start()
    finish(SQUARES, 0, sqs.at[pl.ds(0, R - 1)])
    squares = jnp.sum(sqs[...], axis=0)
    for z in range(STREAMS):
        row = squares[z // group:z // group + 1, :]
        ss = jnp.sum(jnp.where(spot == tok + (z % group) * ALL, row, 0.0), axis=-1, keepdims=True)
        scale = lax.rsqrt(ss / D + EPS)
        n = xb[z].astype(F32).reshape(ALL, WB) * scale * gain_ref[0:1, :]
        nb[z] = n.reshape(R, TOK, WB).astype(BF16)

    rows = SZ * 16
    sc = HD ** -0.5
    ri = lax.broadcasted_iota(jnp.int32, (rows, SZ * 8), 0)
    ci = lax.broadcasted_iota(jnp.int32, (rows, SZ * 8), 1)
    slot = ci % 8
    kvh = jnp.where(ri % 8 >= G, 1, 0)
    new_ok = (ri // 16 == ci // 8) & (slot < STEPS * KH) & (slot % KH == kvh) & (slot // KH <= (ri % 16) // 8)
    per = QH // HALVES
    tile = FF // 4
    half = FF // HALVES

    for l in range(L):
        def qkv(z):
            if l > 0:
                spread_finish(N_ATTN, z, nb)
            if z == 0:
                wwait(l, 0, 1, 2)
            n = nb[z].reshape(ALL, WB)
            col = 0
            for w, width in ((wq, QC), (wk, KC), (wv, KC)):
                put(sbq, z, slice(col, col + width), jnp.dot(n, w[l], preferred_element_type=F32))
                col += width
            sum_start(QKV_B, z, sbq, prq, rbq)

        def attention(z):
            sum_finish(QKV_B, z, sbq, rbq)
            if l == 0:
                spread_finish(X_INIT, z, x)
                if z == 0:
                    finish(GAIN, 0, gains.at[pl.ds(0, R - 1)])
            cos = cos_ref[z]
            sin = sin_ref[z]

            def head(i):
                return total(QKV_B, z, sbq, rbq, slice(i * HD, (i + 1) * HD))

            def rope(v):
                return (v * cos + pltpu.roll(v, HD // 2, 1) * sin).astype(BF16).astype(F32)

            seqs = slice(z * SZ, (z + 1) * SZ)
            for h in range(QH):
                v = rope(head(h))
                for s in range(STEPS):
                    qs[:, s * 8 + h, :] = v[s * SZ:(s + 1) * SZ]
            for h in range(KH):
                v = rope(head(QH + h))
                w = head(QH + KH + h)
                for s in range(STEPS):
                    kn_ref[l, seqs, s * KH + h, :] = v[s * SZ:(s + 1) * SZ]
                    vn_ref[l, seqs, s * KH + h, :] = w[s * SZ:(s + 1) * SZ]

            qall = qs[...].reshape(rows, HD).astype(BF16)
            knew = kn_ref[l, seqs].reshape(SZ * 8, HD).astype(BF16)
            vnew = vn_ref[l, seqs].reshape(SZ * 8, HD).astype(BF16)
            s_new = lax.dot_general(qall, knew, NT, preferred_element_type=F32) * sc
            sn[...] = jnp.where(new_ok, s_new, -jnp.inf).reshape(SZ, 16, SZ * 8)
            if z == 0:
                wwait(l, 3, 4)
            kvrow = jnp.where(lax.broadcasted_iota(jnp.int32, (16, SLOTS), 0) % 8 >= G, 1, 0)
            kcol = lax.broadcasted_iota(jnp.int32, (16, SLOTS), 1)
            parity = (kcol % KH) == kvrow

            def attend(b, carry):
                q = z * SZ + b
                s = lax.dot_general(qs[b].astype(BF16), ck[l, q], NT, preferred_element_type=F32) * sc
                s = jnp.where(parity & (kcol < len_ref[q] * KH), s, -jnp.inf)
                t = sn[b]
                m = jnp.maximum(jnp.max(s, axis=-1, keepdims=True), jnp.max(t, axis=-1, keepdims=True))
                e = jnp.exp(s - m)
                f = jnp.exp(t - m)
                den = jnp.sum(e, axis=-1, keepdims=True) + jnp.sum(f, axis=-1, keepdims=True)
                pn[b] = (f / den).astype(BF16)
                os[b] = jnp.dot((e / den).astype(BF16), cv[l, q], preferred_element_type=F32)
                return carry

            lax.fori_loop(0, SZ, attend, 0, unroll=4)
            o_new = jnp.dot(pn[...].reshape(rows, SZ * 8), vnew, preferred_element_type=F32)
            os[...] = os[...] + o_new.reshape(SZ, 16, HD)
            for h in range(QH):
                o = jnp.concatenate([os[:, s * 8 + h, :] for s in range(STEPS)], axis=0)
                ago[z, own + h // per, :, (h % per) * HD:(h % per + 1) * HD] = o.astype(BF16)
            gather_start(O_COL, z, ago)

        def o_row(z):
            gather_finish(O_COL, z, ago)
            spread_start(O_ROW, z, ago, no)

        def project(act, z, w, depth, ph):
            lhs = act[z].reshape(ALL, depth)
            for h in range(HALVES):
                put(sbo, z, slice(h * WB, (h + 1) * WB),
                    jnp.dot(lhs, w[l, :, h * WB:(h + 1) * WB], preferred_element_type=F32))
            sum_start(ph, z, sbo, pro, rbo)

        def out(z):
            spread_finish(O_ROW, z, no)
            if z == 0:
                wwait(l, 5)
            project(no, z, wo, WB, OUT_B)

        def residual(z, ph, ph_col):
            sum_finish(ph, z, sbo, rbo)
            for h in range(HALVES):
                a = total(ph, z, sbo, rbo, slice(h * WB, (h + 1) * WB))
                x[z, own + h] = (x[z, own + h].astype(F32) + a).astype(BF16)
            gather_start(ph_col, z, x)

        def mlp_norm(z):
            gather_finish(X_MID, z, x)
            norm(z, L + l, False)
            spread_start(N_MLP, z, ns, nb)

        def gate_up(z):
            spread_finish(N_MLP, z, nb)
            if z == 0:
                wwait(l, 6, 7)

            def body(t, carry):
                off = pl.multiple_of(t * tile, tile)
                n = nb[z].reshape(ALL, WB)
                for k, w in enumerate((wg, wu)):
                    put(sbg, z, pl.ds(off + k * FF, tile), jnp.dot(n, w[l, :, pl.ds(off, tile)], preferred_element_type=F32))
                return carry

            lax.fori_loop(0, 4, body, 0)
            sum_start(GU_B, z, sbg, prg, rbg)

        def gate_up_middle(z):
            sum_middle(GU_B, z, sbg, prg, rbg, 8)

        def act(z):
            sum_finish(GU_B, z, sbg, rbg)
            per_half = half // tile

            def body(t, carry):
                off = pl.multiple_of(t * tile, tile)
                g = total(GU_B, z, sbg, rbg, pl.ds(off, tile))
                u = total(GU_B, z, sbg, rbg, pl.ds(off + FF, tile))
                aga[z, own + t // per_half, :, pl.ds(pl.multiple_of((t % per_half) * tile, tile), tile)] = (jax.nn.silu(g) * u).astype(BF16)
                return carry

            lax.fori_loop(0, 4, body, 0)
            gather_start(A_COL, z, aga)

        def a_row(z):
            gather_finish(A_COL, z, aga)
            spread_start(A_ROW, z, aga, na)

        def down(z):
            spread_finish(A_ROW, z, na)
            if z == 0:
                wwait(l, 8)
            project(na, z, wd, half, DOWN_B)

        def end_norm(z):
            gather_finish(X_END, z, x)
            norm(z, l + 1, l == L - 1)
            spread_start(N_ATTN, z, ns, nb)

        stages = [qkv, attention, o_row, out]
        stages += [lambda z: sum_middle(OUT_B, z, sbo, pro, rbo, 1)] if PRE[OUT_B] is not None else []
        stages += [lambda z: residual(z, OUT_B, X_MID), mlp_norm, gate_up, gate_up_middle, act, a_row, down]
        stages += [lambda z: sum_middle(DOWN_B, z, sbo, pro, rbo, 1)] if PRE[DOWN_B] is not None else []
        stages += [lambda z: residual(z, DOWN_B, X_END), end_norm]
        for stage in stages:
            for z in range(STREAMS):
                stage(z)

    for z in range(STREAMS):
        spread_finish(N_ATTN, z, nb)
    for b in range(R):
        v = [nb[z, b].astype(F32) for z in range(STREAMS)]
        for s, out in enumerate((out0, out1)):
            out[b * SEQ:(b + 1) * SEQ] = jnp.concatenate([w[s * SZ:(s + 1) * SZ] for w in v], axis=0).astype(BF16)


def cache_kernel(heads, len_ref, kn_ref, vn_ref, a0, a1, ck_ref, cv_ref, ok_ref, ov_ref, o0, o1,
                 kwin, vwin, bsem, wsem, nsem):
    layers, seqs, rows, width = ck_ref.shape
    sides = ((ck_ref, kwin, kn_ref, ok_ref), (cv_ref, vwin, vn_ref, ov_ref))
    pass_on = [pltpu.make_async_copy(a, b, nsem.at[i]) for i, (a, b) in enumerate(((a0, o0), (a1, o1)))]
    group = seqs // COPY_GROUPS

    def bulk(k, i):
        at = (i // COPY_GROUPS, pl.ds((i % COPY_GROUPS) * group, group))
        return pltpu.make_async_copy(sides[k][0].at[at], sides[k][3].at[at], bsem.at[k, i])

    def place(b):
        at = len_ref[b] * heads
        return at, pl.multiple_of(jnp.minimum((at // 16) * 16, rows - 32), 16)

    def window(k, layer, b):
        return pltpu.make_async_copy(sides[k][1].at[layer, b], sides[k][3].at[layer, b, pl.ds(place(b)[1], 32)], wsem.at[k, layer, b])

    count = layers * COPY_GROUPS
    for i in range(count):
        for k in range(2):
            bulk(k, i).start()
    for cp in pass_on:
        cp.start()

    def patch(b, carry):
        at, base = place(b)
        idx = lax.broadcasted_iota(jnp.int32, (32, width), 0) + base - at
        for layer in range(layers):
            for src, win, fresh, _ in sides:
                val = src[layer, b, pl.ds(base, 32), :].astype(F32)
                new = fresh[layer, b]
                for n in range(STEPS * heads):
                    val = jnp.where(idx == n, new[n:n + 1, :], val)
                win[layer, b] = val.astype(BF16)
        return carry

    lax.fori_loop(0, seqs, patch, 0, unroll=2)
    for i in range(count):
        for k in range(2):
            bulk(k, i).wait()
        for g in range(group):
            for k in range(2):
                window(k, i // COPY_GROUPS, (i % COPY_GROUPS) * group + g).start()
    for cp in pass_on:
        cp.wait()
    for layer in range(layers):
        for b in range(seqs):
            for k in range(2):
                window(k, layer, b).wait()


def solution(mesh):
    R, C = mesh.shape['row'], mesh.shape['col']
    hidden_spec = P('rep', 'row')
    index_spec = P(('rep', 'row'))
    cache_spec = P(None, ('rep', 'row'), None, 'col', None)
    gain_spec = P(None, 'row')
    weight_spec = P(None, 'row', 'col')

    def device_program(hidden_0, hidden_1, positions, lengths, cache_k, cache_v, norm_attn, norm_mlp, w_query, w_key, w_value, w_out, w_gate, w_up, w_down):
        L, SEQ, CTX, KH, HD = cache_k.shape
        WB = hidden_0.shape[1]
        SZ = SEQ // STREAMS
        TOK = SZ * STEPS
        XS = R // CORES
        Z = STREAMS
        QC, KC, FF = w_query.shape[-1], w_key.shape[-1], w_gate.shape[-1]
        HALVES = R // C
        SLOTS = CTX * KH
        ck = cache_k.reshape(L, SEQ, SLOTS, HD)
        cv = cache_v.reshape(L, SEQ, SLOTS, HD)
        vm = pl.BlockSpec(memory_space=pltpu.VMEM)
        smem = pl.BlockSpec(memory_space=pltpu.SMEM)
        hbm = pl.BlockSpec(memory_space=pltpu.HBM)
        weights = (w_query, w_key, w_value, w_out, w_gate, w_up, w_down)
        scratch = [pltpu.VMEM(w.shape, BF16) for w in weights]
        N3 = QC + 2 * KC
        N2 = 2 * FF
        OUTW = HALVES * WB

        def slots(ph):
            return R - 1 if PRE[ph] is None else XS - 1

        scratch += [pltpu.VMEM(s, d) for s, d in (
            ((Z, TOK, HD), F32), ((Z, TOK, HD), F32), ((8, WB), F32), ((8, 128), F32), ((R, 8, 128), F32),
            ((Z, R, TOK, WB), BF16), ((Z, R, TOK, WB), BF16), ((R, 8, WB), F32), ((Z, R, TOK, WB), BF16), ((Z, R, TOK, WB), BF16),
            ((Z, CORES, XS, TOK, N3), BF16), ((Z, XS, TOK, N3), BF16), ((Z, slots(QKV_B), TOK, N3), BF16),
            ((SZ, 16, HD), F32), ((SZ, 16, SZ * 8), F32), ((SZ, 16, SZ * 8), BF16), ((SZ, 16, HD), F32),
            ((Z, R, TOK, WB), BF16), ((Z, R, TOK, WB), BF16),
            ((Z, CORES, XS, TOK, OUTW), BF16), ((Z, XS, TOK, OUTW), BF16), ((Z, slots(OUT_B), TOK, OUTW), BF16),
            ((Z, CORES, XS, TOK, N2), BF16), ((Z, XS, TOK, N2), BF16), ((Z, slots(GU_B), TOK, N2), BF16),
            ((Z, R, TOK, FF // HALVES), BF16), ((Z, R, TOK, FF // HALVES), BF16))]
        scratch += [pltpu.SemaphoreType.DMA((PHASES, Z))] * 2 + [pltpu.SemaphoreType.DMA((L, 9))]
        dims = dict(R=R, C=C, L=L, D=WB * R, HD=HD)
        out_0, out_1, k_new, v_new, kept_k, kept_v = pl.pallas_call(
            functools.partial(decode_kernel, dims),
            out_shape=(pltpu.VMEM(hidden_0.shape, BF16), pltpu.VMEM(hidden_1.shape, BF16),
                       pltpu.VMEM((L, SEQ, 8, HD), F32), pltpu.VMEM((L, SEQ, 8, HD), F32),
                       pltpu.VMEM(ck.shape, BF16), pltpu.VMEM(ck.shape, BF16)),
            in_specs=[vm, vm, smem, smem, vm, vm] + [hbm] * 9,
            out_specs=(vm,) * 6,
            scratch_shapes=scratch,
            compiler_params=pltpu.CompilerParams(collective_id=0, has_side_effects=True, vmem_limit_bytes=47 * 1024 * 1024),
            name='decode',
        )(hidden_0, hidden_1, positions, lengths, norm_attn, norm_mlp, *weights, ck, cv)

        count = L * COPY_GROUPS
        win = pltpu.VMEM((L, SEQ, 32, HD), BF16)
        ok, ov, out_0, out_1 = pl.pallas_call(
            functools.partial(cache_kernel, KH),
            out_shape=(jax.ShapeDtypeStruct(ck.shape, BF16),) * 2 + (jax.ShapeDtypeStruct(hidden_0.shape, BF16),) * 2,
            in_specs=[smem] + [vm] * 6,
            out_specs=(hbm,) * 4,
            scratch_shapes=[win, win, pltpu.SemaphoreType.DMA((2, count)),
                            pltpu.SemaphoreType.DMA((2, L, SEQ)), pltpu.SemaphoreType.DMA((2,))],
            compiler_params=pltpu.CompilerParams(vmem_limit_bytes=8 * 1024 * 1024),
            name='cache_update',
        )(lengths, k_new, v_new, out_0, out_1, kept_k, kept_v)
        ok, ov = ok.reshape(cache_k.shape), ov.reshape(cache_v.shape)
        return out_0, out_1, ok, ov

    return jax.shard_map(device_program, mesh=mesh,
                         in_specs=(hidden_spec, hidden_spec, index_spec, index_spec, cache_spec, cache_spec, gain_spec, gain_spec) + (weight_spec,) * 7,
                         out_specs=(hidden_spec, hidden_spec, cache_spec, cache_spec), check_vma=False)
```

```python
import functools
import math

import jax
import jax.numpy as jnp
from jax import lax
from jax.experimental import pallas as pl
from jax.experimental.pallas import tpu as pltpu
from jax.sharding import PartitionSpec as P

ROPE_BASE = 1000000.0
EPS = 1e-05
F32 = jnp.float32
BF16 = jnp.bfloat16
STEPS = 2
MESH = pl.DeviceIdType.MESH
NT = (((1,), (1,)), ((), ()))

CORES = 2
COPY_GROUPS = 4
PICK = 0
STREAMS = 4

(X_INIT, SQUARES, GAIN, N_ATTN, QKV_A, QKV_B, O_COL, O_ROW, OUT_A, OUT_B, X_MID, N_MLP, GU_A, GU_B, A_COL, A_ROW, DOWN_A, DOWN_B,
 X_END, PHASES) = range(20)
PRE = {QKV_B: None, GU_B: GU_A, OUT_B: None, DOWN_B: None}


COSTS = [(0.4, 0, 1.75, 2.8), (1.9, 1, 0.55, 2.8), (0.2, 0, 0.55, 2.8), (0.4, 0, 1.05, 2.8), (0.3, 1, 0.55, 2.8), (0.4, 0, 0.55, 2.8),
         (1.1, 2, 0.4, 1.1), (0.2, 0, 2.8, 2.8), (0.3, 1, 1.4, 2.8), (0.2, 0, 1.4, 2.8), (0.5, 0, 1.05, 2.8), (0.3, 1, 0.55, 2.8),
         (0.4, 0, 0.55, 2.8)]


def stage_order(layers):
    costs = COSTS * layers
    ready, done, links, now, order = [0.0] * STREAMS, [0] * STREAMS, [0.0] * 3, 0.0, []
    while min(done) < len(costs):
        z = min((k for k in range(STREAMS) if done[k] < len(costs)), key=lambda k: (max(ready[k], now), PICK * done[k], k))
        core, link, wire, latency = costs[done[z]]
        now = max(now, ready[z]) + core
        links[link] = max(links[link], now) + wire
        ready[z] = links[link] + latency
        order.append((done[z], z))
        done[z] += 1
    return order


def decode_kernel(dims, h0, h1, pos_ref, len_ref, ga_ref, gm_ref, wq_h, wk_h, wv_h, wo_h, wg_h, wu_h, wd_h, ck_h, cv_h,
                  out0, out1, kn_ref, vn_ref, ck, cv,
                  wq, wk, wv, wo, wg, wu, wd,
                  cos_ref, sin_ref, gain_ref, sq, sqs, xb, x, gains, ns, nb, sbq, prq, rbq, qs, sn, pn, os, ago, no, sbo, pro, rbo, sbg, prg, rbg, aga, na,
                  ssem, rsem, wsem):
    R, C, L, D = dims['R'], dims['C'], dims['L'], dims['D']
    HD = dims['HD']
    SEQ = h0.shape[0] // R
    SZ = SEQ // STREAMS
    TOK = SZ * STEPS
    ALL = TOK * R
    WB = h0.shape[1]
    QC, KC = wq.shape[-1], wk.shape[-1]
    QH, KH = QC // HD, KC // HD
    G = QH // KH
    FF = wg.shape[-1]
    HALVES = R // C
    SLOTS = ck.shape[2]
    XS = R // CORES
    r = lax.axis_index('row')
    c = lax.axis_index('col')
    chip, core = lax.div(r, CORES), lax.rem(r, CORES)
    own = c * HALVES
    mine = pl.ds(own, HALVES)

    pairs = [(wq_h, wq), (wk_h, wk), (wv_h, wv), (ck_h, ck), (cv_h, cv), (wo_h, wo), (wg_h, wg), (wu_h, wu), (wd_h, wd)]

    def fetch(layer, i):
        return pltpu.make_async_copy(pairs[i][0].at[layer], pairs[i][1].at[layer], wsem.at[layer, i])

    waited = set()

    def wwait(layer, *which):
        for i in which:
            if (layer, i) not in waited:
                waited.add((layer, i))
                fetch(layer, i).wait()

    for i in range(len(pairs)):
        fetch(0, i).start()

    barrier = pltpu.get_barrier_semaphore()
    for j in range(1, R):
        pl.semaphore_signal(barrier, inc=1, device_id={'row': lax.rem(r + j, R)}, device_id_type=MESH)
    for j in range(1, C):
        pl.semaphore_signal(barrier, inc=1, device_id={'col': lax.rem(c + j, C)}, device_id_type=MESH)

    def remote(ph, z, src, dst, device):
        pltpu.make_async_remote_copy(src_ref=src, dst_ref=dst, send_sem=ssem.at[ph, z], recv_sem=rsem.at[ph, z],
                                     device_id=device, device_id_type=MESH).start()

    def finish(ph, z, received):
        pltpu.make_async_copy(received, received, rsem.at[ph, z]).wait()
        pltpu.make_async_copy(received, received, ssem.at[ph, z]).wait()

    def row_send(ph, z, src, dst):
        for j in range(1, R):
            peer = lax.rem(r + j, R)
            remote(ph, z, src(peer), dst(j), {'row': peer})

    def spread_start(ph, z, src, dst):
        row_send(ph, z, lambda peer: src.at[z, peer], lambda j: dst.at[z, r])
        dst[z, r] = src[z, r]

    def spread_finish(ph, z, dst):
        finish(ph, z, dst.at[z, pl.ds(0, R - 1)])

    def gather_start(ph, z, buf):
        for j in range(1, C):
            remote(ph, z, buf.at[z, mine], buf.at[z, mine], {'col': lax.rem(c + j, C)})

    def gather_finish(ph, z, buf):
        finish(ph, z, buf.at[z, pl.ds(0, (C - 1) * HALVES)])

    def sum_start(ph, z, sb, pr, rb):
        if PRE[ph] is not None:
            remote(PRE[ph], z, sb.at[z, 1 - core], pr.at[z], {'row': r + 1 - 2 * core})
        else:
            row_send(ph, z, lambda peer: sb.at[z, lax.rem(peer, CORES), lax.div(peer, CORES)], lambda j: rb.at[z, j - 1])

    def sum_middle(ph, z, sb, pr, rb, tiles):
        if PRE[ph] is None:
            return
        finish(PRE[ph], z, pr.at[z])
        width = sb.shape[-1] // tiles

        def add(t, carry):
            sl = pl.ds(pl.multiple_of(t * width, width), width)
            sb[z, core, :, :, sl] = (sb[z, core, :, :, sl].astype(F32) + pr[z, :, :, sl].astype(F32)).astype(BF16)
            return carry

        lax.fori_loop(0, tiles, add, 0)
        for j in range(1, XS):
            peer = lax.rem(chip + j, XS)
            remote(ph, z, sb.at[z, core, peer], rb.at[z, j - 1], {'row': peer * CORES + core})

    def sum_finish(ph, z, sb, rb):
        finish(ph, z, rb.at[z])

    def total(ph, z, sb, rb, sl):
        a = sb[z, core, chip, :, sl].astype(F32)
        for j in range((XS if PRE[ph] is not None else R) - 1):
            a = a + rb[z, j, :, sl].astype(F32)
        return a.astype(BF16).astype(F32)

    def put(sb, z, cols, res):
        v = res.astype(BF16).reshape(XS, CORES, TOK, res.shape[-1])
        for k in range(CORES):
            sb[z, k, :, :, cols] = v[:, k]

    def norm(z, gi, last):
        ss = jnp.zeros((TOK, 1), F32)
        for k in range(R):
            xk = x[z, k].astype(F32)
            ss = ss + jnp.sum(xk * xk, axis=-1, keepdims=True)
        scale = lax.rsqrt(ss / D + EPS)
        for k in range(R):
            xk = x[z, k].astype(F32)
            n = xk if last else xk * scale * gains[k, gi:gi + 1, :]
            ns[z, k] = n.astype(BF16)

    gain_ref[...] = jnp.zeros_like(gain_ref)
    gain_ref[0:L] = ga_ref[...].astype(F32)
    gain_ref[L:2 * L] = gm_ref[...].astype(F32)
    lane = lax.broadcasted_iota(jnp.int32, (TOK, HD), 1)
    token = lax.broadcasted_iota(jnp.int32, (TOK, HD), 0)
    half_lane = lax.rem(lane, HD // 2)
    inv_freq = jnp.exp(half_lane.astype(F32) * (-2.0 / HD * math.log(ROPE_BASE)))
    for z in range(STREAMS):
        position = jnp.zeros((TOK, HD), jnp.int32)
        for b in range(SZ):
            position = jnp.where(lax.rem(token, SZ) == b, pos_ref[z * SZ + b], position)
        angle = (position + lax.div(token, SZ)).astype(F32) * inv_freq
        cos_ref[z] = jnp.cos(angle)
        sine = jnp.sin(angle)
        sin_ref[z] = jnp.where(lane < HD // 2, -sine, sine)

    for b in range(R):
        v0 = h0[b * SEQ:(b + 1) * SEQ].astype(F32)
        v1 = h1[b * SEQ:(b + 1) * SEQ].astype(F32)
        for z in range(STREAMS):
            part = slice(z * SZ, (z + 1) * SZ)
            xb[z, b] = jnp.concatenate([v0[part], v1[part]], axis=0).astype(BF16)
    qs[...] = jnp.zeros_like(qs)
    kn_ref[...] = jnp.zeros_like(kn_ref)
    vn_ref[...] = jnp.zeros_like(vn_ref)
    pl.semaphore_wait(barrier, R + C - 2)

    group = 128 // ALL
    tok = lax.broadcasted_iota(jnp.int32, (ALL, 128), 0)
    spot = lax.broadcasted_iota(jnp.int32, (ALL, 128), 1)
    line = lax.broadcasted_iota(jnp.int32, (8, 128), 0)
    packed = jnp.zeros((8, 128), F32)
    for z in range(STREAMS):
        xz = xb[z].astype(F32).reshape(ALL, WB)
        ss = jnp.sum(xz * xz, axis=-1, keepdims=True)
        lanes = jnp.sum(jnp.where(spot == tok + (z % group) * ALL, ss, 0.0), axis=0, keepdims=True)
        packed = packed + jnp.where(line == z // group, lanes, 0.0)
    sq[...] = packed
    row_send(SQUARES, 0, lambda peer: sq, lambda j: sqs.at[r])
    sqs[r] = sq[...]
    row_send(GAIN, 0, lambda peer: gain_ref, lambda j: gains.at[r])
    gains[r] = gain_ref[...]
    for z in range(STREAMS):
        spread_start(X_INIT, z, xb, x)
    for layer in range(1, L):
        for i in range(len(pairs)):
            fetch(layer, i).start()
    finish(SQUARES, 0, sqs.at[pl.ds(0, R - 1)])
    squares = jnp.sum(sqs[...], axis=0)
    for z in range(STREAMS):
        row = squares[z // group:z // group + 1, :]
        ss = jnp.sum(jnp.where(spot == tok + (z % group) * ALL, row, 0.0), axis=-1, keepdims=True)
        scale = lax.rsqrt(ss / D + EPS)
        n = xb[z].astype(F32).reshape(ALL, WB) * scale * gain_ref[0:1, :]
        nb[z] = n.reshape(R, TOK, WB).astype(BF16)

    rows = SZ * 16
    sc = HD ** -0.5
    ri = lax.broadcasted_iota(jnp.int32, (rows, SZ * 8), 0)
    ci = lax.broadcasted_iota(jnp.int32, (rows, SZ * 8), 1)
    slot = ci % 8
    kvh = jnp.where(ri % 8 >= G, 1, 0)
    new_ok = (ri // 16 == ci // 8) & (slot < STEPS * KH) & (slot % KH == kvh) & (slot // KH <= (ri % 16) // 8)
    per = QH // HALVES
    tile = FF // 4
    half = FF // HALVES

    def layer_stages(l):
        def qkv(z):
            if l > 0:
                spread_finish(N_ATTN, z, nb)
            wwait(l, 0, 1, 2)
            n = nb[z].reshape(ALL, WB)
            col = 0
            for w, width in ((wq, QC), (wk, KC), (wv, KC)):
                put(sbq, z, slice(col, col + width), jnp.dot(n, w[l], preferred_element_type=F32))
                col += width
            sum_start(QKV_B, z, sbq, prq, rbq)

        def attention(z):
            sum_finish(QKV_B, z, sbq, rbq)
            if l == 0:
                spread_finish(X_INIT, z, x)
                if not waited & {GAIN}:
                    waited.add(GAIN)
                    finish(GAIN, 0, gains.at[pl.ds(0, R - 1)])
            cos = cos_ref[z]
            sin = sin_ref[z]

            def head(i):
                return total(QKV_B, z, sbq, rbq, slice(i * HD, (i + 1) * HD))

            def rope(v):
                return (v * cos + pltpu.roll(v, HD // 2, 1) * sin).astype(BF16).astype(F32)

            seqs = slice(z * SZ, (z + 1) * SZ)
            for h in range(QH):
                v = rope(head(h))
                for s in range(STEPS):
                    qs[:, s * 8 + h, :] = v[s * SZ:(s + 1) * SZ]
            for h in range(KH):
                v = rope(head(QH + h))
                w = head(QH + KH + h)
                for s in range(STEPS):
                    kn_ref[l, seqs, s * KH + h, :] = v[s * SZ:(s + 1) * SZ]
                    vn_ref[l, seqs, s * KH + h, :] = w[s * SZ:(s + 1) * SZ]

            qall = qs[...].reshape(rows, HD).astype(BF16)
            knew = kn_ref[l, seqs].reshape(SZ * 8, HD).astype(BF16)
            vnew = vn_ref[l, seqs].reshape(SZ * 8, HD).astype(BF16)
            s_new = lax.dot_general(qall, knew, NT, preferred_element_type=F32) * sc
            sn[...] = jnp.where(new_ok, s_new, -jnp.inf).reshape(SZ, 16, SZ * 8)
            wwait(l, 3, 4)
            kvrow = jnp.where(lax.broadcasted_iota(jnp.int32, (16, SLOTS), 0) % 8 >= G, 1, 0)
            kcol = lax.broadcasted_iota(jnp.int32, (16, SLOTS), 1)
            parity = (kcol % KH) == kvrow

            def attend(b, carry):
                q = z * SZ + b
                s = lax.dot_general(qs[b].astype(BF16), ck[l, q], NT, preferred_element_type=F32) * sc
                s = jnp.where(parity & (kcol < len_ref[q] * KH), s, -jnp.inf)
                t = sn[b]
                m = jnp.maximum(jnp.max(s, axis=-1, keepdims=True), jnp.max(t, axis=-1, keepdims=True))
                e = jnp.exp(s - m)
                f = jnp.exp(t - m)
                den = jnp.sum(e, axis=-1, keepdims=True) + jnp.sum(f, axis=-1, keepdims=True)
                pn[b] = (f / den).astype(BF16)
                os[b] = jnp.dot((e / den).astype(BF16), cv[l, q], preferred_element_type=F32)
                return carry

            lax.fori_loop(0, SZ, attend, 0, unroll=4)
            o_new = jnp.dot(pn[...].reshape(rows, SZ * 8), vnew, preferred_element_type=F32)
            os[...] = os[...] + o_new.reshape(SZ, 16, HD)
            for h in range(QH):
                o = jnp.concatenate([os[:, s * 8 + h, :] for s in range(STEPS)], axis=0)
                ago[z, own + h // per, :, (h % per) * HD:(h % per + 1) * HD] = o.astype(BF16)
            gather_start(O_COL, z, ago)

        def o_row(z):
            gather_finish(O_COL, z, ago)
            spread_start(O_ROW, z, ago, no)

        def project(act, z, w, depth, ph):
            lhs = act[z].reshape(ALL, depth)
            for h in range(HALVES):
                put(sbo, z, slice(h * WB, (h + 1) * WB),
                    jnp.dot(lhs, w[l, :, h * WB:(h + 1) * WB], preferred_element_type=F32))
            sum_start(ph, z, sbo, pro, rbo)

        def out(z):
            spread_finish(O_ROW, z, no)
            wwait(l, 5)
            project(no, z, wo, WB, OUT_B)

        def residual(z, ph, ph_col):
            sum_finish(ph, z, sbo, rbo)
            for h in range(HALVES):
                a = total(ph, z, sbo, rbo, slice(h * WB, (h + 1) * WB))
                x[z, own + h] = (x[z, own + h].astype(F32) + a).astype(BF16)
            gather_start(ph_col, z, x)

        def mlp_norm(z):
            gather_finish(X_MID, z, x)
            norm(z, L + l, False)
            spread_start(N_MLP, z, ns, nb)

        def gate_up(z):
            spread_finish(N_MLP, z, nb)
            wwait(l, 6, 7)

            def body(t, carry):
                off = pl.multiple_of(t * tile, tile)
                n = nb[z].reshape(ALL, WB)
                for k, w in enumerate((wg, wu)):
                    put(sbg, z, pl.ds(off + k * FF, tile), jnp.dot(n, w[l, :, pl.ds(off, tile)], preferred_element_type=F32))
                return carry

            lax.fori_loop(0, 4, body, 0)
            sum_start(GU_B, z, sbg, prg, rbg)

        def gate_up_middle(z):
            sum_middle(GU_B, z, sbg, prg, rbg, 8)

        def act(z):
            sum_finish(GU_B, z, sbg, rbg)
            per_half = half // tile

            def body(t, carry):
                off = pl.multiple_of(t * tile, tile)
                g = total(GU_B, z, sbg, rbg, pl.ds(off, tile))
                u = total(GU_B, z, sbg, rbg, pl.ds(off + FF, tile))
                aga[z, own + t // per_half, :, pl.ds(pl.multiple_of((t % per_half) * tile, tile), tile)] = (jax.nn.silu(g) * u).astype(BF16)
                return carry

            lax.fori_loop(0, 4, body, 0)
            gather_start(A_COL, z, aga)

        def a_row(z):
            gather_finish(A_COL, z, aga)
            spread_start(A_ROW, z, aga, na)

        def down(z):
            spread_finish(A_ROW, z, na)
            wwait(l, 8)
            project(na, z, wd, half, DOWN_B)

        def end_norm(z):
            gather_finish(X_END, z, x)
            norm(z, l + 1, l == L - 1)
            spread_start(N_ATTN, z, ns, nb)

        stages = [qkv, attention, o_row, out]
        stages += [lambda z: sum_middle(OUT_B, z, sbo, pro, rbo, 1)] if PRE[OUT_B] is not None else []
        stages += [lambda z: residual(z, OUT_B, X_MID), mlp_norm, gate_up, gate_up_middle, act, a_row, down]
        stages += [lambda z: sum_middle(DOWN_B, z, sbo, pro, rbo, 1)] if PRE[DOWN_B] is not None else []
        stages += [lambda z: residual(z, DOWN_B, X_END), end_norm]
        return stages

    stages = [stage for l in range(L) for stage in layer_stages(l)]
    for i, z in stage_order(L):
        stages[i](z)
    for z in range(STREAMS):
        spread_finish(N_ATTN, z, nb)
    for b in range(R):
        v = [nb[z, b].astype(F32) for z in range(STREAMS)]
        for s, out in enumerate((out0, out1)):
            out[b * SEQ:(b + 1) * SEQ] = jnp.concatenate([w[s * SZ:(s + 1) * SZ] for w in v], axis=0).astype(BF16)


def cache_kernel(heads, len_ref, kn_ref, vn_ref, a0, a1, ck_ref, cv_ref, ok_ref, ov_ref, o0, o1,
                 kwin, vwin, bsem, wsem, nsem):
    layers, seqs, rows, width = ck_ref.shape
    sides = ((ck_ref, kwin, kn_ref, ok_ref), (cv_ref, vwin, vn_ref, ov_ref))
    pass_on = [pltpu.make_async_copy(a, b, nsem.at[i]) for i, (a, b) in enumerate(((a0, o0), (a1, o1)))]
    group = seqs // COPY_GROUPS

    def bulk(k, i):
        at = (i // COPY_GROUPS, pl.ds((i % COPY_GROUPS) * group, group))
        return pltpu.make_async_copy(sides[k][0].at[at], sides[k][3].at[at], bsem.at[k, i])

    def place(b):
        at = len_ref[b] * heads
        return at, pl.multiple_of(jnp.minimum((at // 16) * 16, rows - 32), 16)

    def window(k, layer, b):
        return pltpu.make_async_copy(sides[k][1].at[layer, b], sides[k][3].at[layer, b, pl.ds(place(b)[1], 32)], wsem.at[k, layer, b])

    count = layers * COPY_GROUPS
    for i in range(count):
        for k in range(2):
            bulk(k, i).start()
    for cp in pass_on:
        cp.start()

    def patch(b, carry):
        at, base = place(b)
        idx = lax.broadcasted_iota(jnp.int32, (32, width), 0) + base - at
        for layer in range(layers):
            for src, win, fresh, _ in sides:
                val = src[layer, b, pl.ds(base, 32), :].astype(F32)
                new = fresh[layer, b]
                for n in range(STEPS * heads):
                    val = jnp.where(idx == n, new[n:n + 1, :], val)
                win[layer, b] = val.astype(BF16)
        return carry

    lax.fori_loop(0, seqs, patch, 0, unroll=2)
    for i in range(count):
        for k in range(2):
            bulk(k, i).wait()
        for g in range(group):
            for k in range(2):
                window(k, i // COPY_GROUPS, (i % COPY_GROUPS) * group + g).start()
    for cp in pass_on:
        cp.wait()
    for layer in range(layers):
        for b in range(seqs):
            for k in range(2):
                window(k, layer, b).wait()


def solution(mesh):
    R, C = mesh.shape['row'], mesh.shape['col']
    hidden_spec = P('rep', 'row')
    index_spec = P(('rep', 'row'))
    cache_spec = P(None, ('rep', 'row'), None, 'col', None)
    gain_spec = P(None, 'row')
    weight_spec = P(None, 'row', 'col')

    def device_program(hidden_0, hidden_1, positions, lengths, cache_k, cache_v, norm_attn, norm_mlp, w_query, w_key, w_value, w_out, w_gate, w_up, w_down):
        L, SEQ, CTX, KH, HD = cache_k.shape
        WB = hidden_0.shape[1]
        SZ = SEQ // STREAMS
        TOK = SZ * STEPS
        XS = R // CORES
        Z = STREAMS
        QC, KC, FF = w_query.shape[-1], w_key.shape[-1], w_gate.shape[-1]
        HALVES = R // C
        SLOTS = CTX * KH
        ck = cache_k.reshape(L, SEQ, SLOTS, HD)
        cv = cache_v.reshape(L, SEQ, SLOTS, HD)
        vm = pl.BlockSpec(memory_space=pltpu.VMEM)
        smem = pl.BlockSpec(memory_space=pltpu.SMEM)
        hbm = pl.BlockSpec(memory_space=pltpu.HBM)
        weights = (w_query, w_key, w_value, w_out, w_gate, w_up, w_down)
        scratch = [pltpu.VMEM(w.shape, BF16) for w in weights]
        N3 = QC + 2 * KC
        N2 = 2 * FF
        OUTW = HALVES * WB

        def slots(ph):
            return R - 1 if PRE[ph] is None else XS - 1

        scratch += [pltpu.VMEM(s, d) for s, d in (
            ((Z, TOK, HD), F32), ((Z, TOK, HD), F32), ((8, WB), F32), ((8, 128), F32), ((R, 8, 128), F32),
            ((Z, R, TOK, WB), BF16), ((Z, R, TOK, WB), BF16), ((R, 8, WB), F32), ((Z, R, TOK, WB), BF16), ((Z, R, TOK, WB), BF16),
            ((Z, CORES, XS, TOK, N3), BF16), ((Z, XS, TOK, N3), BF16), ((Z, slots(QKV_B), TOK, N3), BF16),
            ((SZ, 16, HD), F32), ((SZ, 16, SZ * 8), F32), ((SZ, 16, SZ * 8), BF16), ((SZ, 16, HD), F32),
            ((Z, R, TOK, WB), BF16), ((Z, R, TOK, WB), BF16),
            ((Z, CORES, XS, TOK, OUTW), BF16), ((Z, XS, TOK, OUTW), BF16), ((Z, slots(OUT_B), TOK, OUTW), BF16),
            ((Z, CORES, XS, TOK, N2), BF16), ((Z, XS, TOK, N2), BF16), ((Z, slots(GU_B), TOK, N2), BF16),
            ((Z, R, TOK, FF // HALVES), BF16), ((Z, R, TOK, FF // HALVES), BF16))]
        scratch += [pltpu.SemaphoreType.DMA((PHASES, Z))] * 2 + [pltpu.SemaphoreType.DMA((L, 9))]
        dims = dict(R=R, C=C, L=L, D=WB * R, HD=HD)
        out_0, out_1, k_new, v_new, kept_k, kept_v = pl.pallas_call(
            functools.partial(decode_kernel, dims),
            out_shape=(pltpu.VMEM(hidden_0.shape, BF16), pltpu.VMEM(hidden_1.shape, BF16),
                       pltpu.VMEM((L, SEQ, 8, HD), F32), pltpu.VMEM((L, SEQ, 8, HD), F32),
                       pltpu.VMEM(ck.shape, BF16), pltpu.VMEM(ck.shape, BF16)),
            in_specs=[vm, vm, smem, smem, vm, vm] + [hbm] * 9,
            out_specs=(vm,) * 6,
            scratch_shapes=scratch,
            compiler_params=pltpu.CompilerParams(collective_id=0, has_side_effects=True, vmem_limit_bytes=47 * 1024 * 1024),
            name='decode',
        )(hidden_0, hidden_1, positions, lengths, norm_attn, norm_mlp, *weights, ck, cv)

        count = L * COPY_GROUPS
        win = pltpu.VMEM((L, SEQ, 32, HD), BF16)
        ok, ov, out_0, out_1 = pl.pallas_call(
            functools.partial(cache_kernel, KH),
            out_shape=(jax.ShapeDtypeStruct(ck.shape, BF16),) * 2 + (jax.ShapeDtypeStruct(hidden_0.shape, BF16),) * 2,
            in_specs=[smem] + [vm] * 6,
            out_specs=(hbm,) * 4,
            scratch_shapes=[win, win, pltpu.SemaphoreType.DMA((2, count)),
                            pltpu.SemaphoreType.DMA((2, L, SEQ)), pltpu.SemaphoreType.DMA((2,))],
            compiler_params=pltpu.CompilerParams(vmem_limit_bytes=8 * 1024 * 1024),
            name='cache_update',
        )(lengths, k_new, v_new, out_0, out_1, kept_k, kept_v)
        ok, ov = ok.reshape(cache_k.shape), ov.reshape(cache_v.shape)
        return out_0, out_1, ok, ov

    return jax.shard_map(device_program, mesh=mesh,
                         in_specs=(hidden_spec, hidden_spec, index_spec, index_spec, cache_spec, cache_spec, gain_spec, gain_spec) + (weight_spec,) * 7,
                         out_specs=(hidden_spec, hidden_spec, cache_spec, cache_spec), check_vma=False)
```

```python
import functools
import math

import jax
import jax.numpy as jnp
from jax import lax
from jax.experimental import pallas as pl
from jax.experimental.pallas import tpu as pltpu
from jax.sharding import PartitionSpec as P

ROPE_BASE = 1000000.0
EPS = 1e-05
F32 = jnp.float32
BF16 = jnp.bfloat16
STEPS = 2
MESH = pl.DeviceIdType.MESH
NT = (((1,), (1,)), ((), ()))

CORES = 2
COPY_GROUPS = 4
PICK = 0
STREAMS = 4

(X_INIT, SQUARES, GAIN, N_ATTN, QKV_A, QKV_B, O_COL, O_ROW, OUT_A, OUT_B, X_MID, N_MLP, GU_A, GU_B, A_COL, A_ROW, DOWN_A, DOWN_B,
 X_END, PHASES) = range(20)
PRE = {QKV_B: None, GU_B: GU_A, OUT_B: None, DOWN_B: None}


COSTS = [(0.4, 0, 1.75, 2.8), (1.9, 1, 0.55, 2.8), (0.2, 0, 0.55, 2.8), (0.4, 0, 1.05, 2.8), (0.3, 1, 0.55, 2.8), (0.4, 0, 0.55, 2.8),
         (1.1, 2, 0.4, 1.1), (0.2, 0, 2.8, 2.8), (0.3, 1, 1.4, 2.8), (0.2, 0, 1.4, 2.8), (0.5, 0, 1.05, 2.8), (0.3, 1, 0.55, 2.8),
         (0.4, 0, 0.55, 2.8)]


def far_first(n):
    return sorted(range(1, n), key=lambda j: -min(j, n - j))


def stage_order(layers):
    costs = COSTS * layers
    ready, done, links, now, order = [0.0] * STREAMS, [0] * STREAMS, [0.0] * 3, 0.0, []
    while min(done) < len(costs):
        z = min((k for k in range(STREAMS) if done[k] < len(costs)), key=lambda k: (max(ready[k], now), PICK * done[k], k))
        core, link, wire, latency = costs[done[z]]
        now = max(now, ready[z]) + core
        links[link] = max(links[link], now) + wire
        ready[z] = links[link] + latency
        order.append((done[z], z))
        done[z] += 1
    return order


def decode_kernel(dims, h0, h1, pos_ref, len_ref, ga_ref, gm_ref, wq_h, wk_h, wv_h, wo_h, wg_h, wu_h, wd_h, ck_h, cv_h,
                  out0, out1, kn_ref, vn_ref, ck, cv,
                  wq, wk, wv, wo, wg, wu, wd,
                  cos_ref, sin_ref, gain_ref, sq, sqs, xb, x, gains, ns, nb, sbq, prq, rbq, qs, sn, pn, os, ago, no, sbo, pro, rbo, sbg, prg, rbg, aga, na,
                  ssem, rsem, wsem):
    R, C, L, D = dims['R'], dims['C'], dims['L'], dims['D']
    HD = dims['HD']
    SEQ = h0.shape[0] // R
    SZ = SEQ // STREAMS
    TOK = SZ * STEPS
    ALL = TOK * R
    WB = h0.shape[1]
    QC, KC = wq.shape[-1], wk.shape[-1]
    QH, KH = QC // HD, KC // HD
    G = QH // KH
    FF = wg.shape[-1]
    HALVES = R // C
    SLOTS = ck.shape[2]
    XS = R // CORES
    r = lax.axis_index('row')
    c = lax.axis_index('col')
    chip, core = lax.div(r, CORES), lax.rem(r, CORES)
    own = c * HALVES
    mine = pl.ds(own, HALVES)

    pairs = [(wq_h, wq), (wk_h, wk), (wv_h, wv), (ck_h, ck), (cv_h, cv), (wo_h, wo), (wg_h, wg), (wu_h, wu), (wd_h, wd)]

    def fetch(layer, i):
        return pltpu.make_async_copy(pairs[i][0].at[layer], pairs[i][1].at[layer], wsem.at[layer, i])

    waited = set()

    def wwait(layer, *which):
        for i in which:
            if (layer, i) not in waited:
                waited.add((layer, i))
                fetch(layer, i).wait()

    for i in range(len(pairs)):
        fetch(0, i).start()

    barrier = pltpu.get_barrier_semaphore()
    for j in range(1, R):
        pl.semaphore_signal(barrier, inc=1, device_id={'row': lax.rem(r + j, R)}, device_id_type=MESH)
    for j in range(1, C):
        pl.semaphore_signal(barrier, inc=1, device_id={'col': lax.rem(c + j, C)}, device_id_type=MESH)

    def remote(ph, z, src, dst, device):
        pltpu.make_async_remote_copy(src_ref=src, dst_ref=dst, send_sem=ssem.at[ph, z], recv_sem=rsem.at[ph, z],
                                     device_id=device, device_id_type=MESH).start()

    def finish(ph, z, received):
        pltpu.make_async_copy(received, received, rsem.at[ph, z]).wait()
        pltpu.make_async_copy(received, received, ssem.at[ph, z]).wait()

    def row_send(ph, z, src, dst):
        for j in far_first(R):
            peer = lax.rem(r + j, R)
            remote(ph, z, src(peer), dst(j), {'row': peer})

    def spread_start(ph, z, src, dst):
        row_send(ph, z, lambda peer: src.at[z, peer], lambda j: dst.at[z, r])
        dst[z, r] = src[z, r]

    def spread_finish(ph, z, dst):
        finish(ph, z, dst.at[z, pl.ds(0, R - 1)])

    def gather_start(ph, z, buf):
        for j in far_first(C):
            remote(ph, z, buf.at[z, mine], buf.at[z, mine], {'col': lax.rem(c + j, C)})

    def gather_finish(ph, z, buf):
        finish(ph, z, buf.at[z, pl.ds(0, (C - 1) * HALVES)])

    def sum_start(ph, z, sb, pr, rb):
        if PRE[ph] is not None:
            remote(PRE[ph], z, sb.at[z, 1 - core], pr.at[z], {'row': r + 1 - 2 * core})
        else:
            row_send(ph, z, lambda peer: sb.at[z, lax.rem(peer, CORES), lax.div(peer, CORES)], lambda j: rb.at[z, j - 1])

    def sum_middle(ph, z, sb, pr, rb, tiles):
        if PRE[ph] is None:
            return
        finish(PRE[ph], z, pr.at[z])
        width = sb.shape[-1] // tiles

        def add(t, carry):
            sl = pl.ds(pl.multiple_of(t * width, width), width)
            sb[z, core, :, :, sl] = (sb[z, core, :, :, sl].astype(F32) + pr[z, :, :, sl].astype(F32)).astype(BF16)
            return carry

        lax.fori_loop(0, tiles, add, 0)
        for j in far_first(XS):
            peer = lax.rem(chip + j, XS)
            remote(ph, z, sb.at[z, core, peer], rb.at[z, j - 1], {'row': peer * CORES + core})

    def sum_finish(ph, z, sb, rb):
        finish(ph, z, rb.at[z])

    def total(ph, z, sb, rb, sl):
        a = sb[z, core, chip, :, sl].astype(F32)
        for j in range((XS if PRE[ph] is not None else R) - 1):
            a = a + rb[z, j, :, sl].astype(F32)
        return a.astype(BF16).astype(F32)

    def put(sb, z, cols, res):
        v = res.astype(BF16).reshape(XS, CORES, TOK, res.shape[-1])
        for k in range(CORES):
            sb[z, k, :, :, cols] = v[:, k]

    def norm(z, gi, last):
        ss = jnp.zeros((TOK, 1), F32)
        for k in range(R):
            xk = x[z, k].astype(F32)
            ss = ss + jnp.sum(xk * xk, axis=-1, keepdims=True)
        scale = lax.rsqrt(ss / D + EPS)
        for k in range(R):
            xk = x[z, k].astype(F32)
            n = xk if last else xk * scale * gains[k, gi:gi + 1, :]
            ns[z, k] = n.astype(BF16)

    gain_ref[...] = jnp.zeros_like(gain_ref)
    gain_ref[0:L] = ga_ref[...].astype(F32)
    gain_ref[L:2 * L] = gm_ref[...].astype(F32)
    lane = lax.broadcasted_iota(jnp.int32, (TOK, HD), 1)
    token = lax.broadcasted_iota(jnp.int32, (TOK, HD), 0)
    half_lane = lax.rem(lane, HD // 2)
    inv_freq = jnp.exp(half_lane.astype(F32) * (-2.0 / HD * math.log(ROPE_BASE)))
    for z in range(STREAMS):
        position = jnp.zeros((TOK, HD), jnp.int32)
        for b in range(SZ):
            position = jnp.where(lax.rem(token, SZ) == b, pos_ref[z * SZ + b], position)
        angle = (position + lax.div(token, SZ)).astype(F32) * inv_freq
        cos_ref[z] = jnp.cos(angle)
        sine = jnp.sin(angle)
        sin_ref[z] = jnp.where(lane < HD // 2, -sine, sine)

    for b in range(R):
        v0 = h0[b * SEQ:(b + 1) * SEQ].astype(F32)
        v1 = h1[b * SEQ:(b + 1) * SEQ].astype(F32)
        for z in range(STREAMS):
            part = slice(z * SZ, (z + 1) * SZ)
            xb[z, b] = jnp.concatenate([v0[part], v1[part]], axis=0).astype(BF16)
    qs[...] = jnp.zeros_like(qs)
    kn_ref[...] = jnp.zeros_like(kn_ref)
    vn_ref[...] = jnp.zeros_like(vn_ref)
    pl.semaphore_wait(barrier, R + C - 2)

    group = 128 // ALL
    tok = lax.broadcasted_iota(jnp.int32, (ALL, 128), 0)
    spot = lax.broadcasted_iota(jnp.int32, (ALL, 128), 1)
    line = lax.broadcasted_iota(jnp.int32, (8, 128), 0)
    packed = jnp.zeros((8, 128), F32)
    for z in range(STREAMS):
        xz = xb[z].astype(F32).reshape(ALL, WB)
        ss = jnp.sum(xz * xz, axis=-1, keepdims=True)
        lanes = jnp.sum(jnp.where(spot == tok + (z % group) * ALL, ss, 0.0), axis=0, keepdims=True)
        packed = packed + jnp.where(line == z // group, lanes, 0.0)
    sq[...] = packed
    row_send(SQUARES, 0, lambda peer: sq, lambda j: sqs.at[r])
    sqs[r] = sq[...]
    row_send(GAIN, 0, lambda peer: gain_ref, lambda j: gains.at[r])
    gains[r] = gain_ref[...]
    for z in range(STREAMS):
        spread_start(X_INIT, z, xb, x)
    for layer in range(1, L):
        for i in range(len(pairs)):
            fetch(layer, i).start()
    finish(SQUARES, 0, sqs.at[pl.ds(0, R - 1)])
    squares = jnp.sum(sqs[...], axis=0)
    for z in range(STREAMS):
        row = squares[z // group:z // group + 1, :]
        ss = jnp.sum(jnp.where(spot == tok + (z % group) * ALL, row, 0.0), axis=-1, keepdims=True)
        scale = lax.rsqrt(ss / D + EPS)
        n = xb[z].astype(F32).reshape(ALL, WB) * scale * gain_ref[0:1, :]
        nb[z] = n.reshape(R, TOK, WB).astype(BF16)

    rows = SZ * 16
    sc = HD ** -0.5
    ri = lax.broadcasted_iota(jnp.int32, (rows, SZ * 8), 0)
    ci = lax.broadcasted_iota(jnp.int32, (rows, SZ * 8), 1)
    slot = ci % 8
    kvh = jnp.where(ri % 8 >= G, 1, 0)
    new_ok = (ri // 16 == ci // 8) & (slot < STEPS * KH) & (slot % KH == kvh) & (slot // KH <= (ri % 16) // 8)
    per = QH // HALVES
    tile = FF // 2
    half = FF // HALVES

    def layer_stages(l):
        def qkv(z):
            if l > 0:
                spread_finish(N_ATTN, z, nb)
            wwait(l, 0, 1, 2)
            n = nb[z].reshape(ALL, WB)
            col = 0
            for w, width in ((wq, QC), (wk, KC), (wv, KC)):
                put(sbq, z, slice(col, col + width), jnp.dot(n, w[l], preferred_element_type=F32))
                col += width
            sum_start(QKV_B, z, sbq, prq, rbq)

        def attention(z):
            sum_finish(QKV_B, z, sbq, rbq)
            if l == 0:
                spread_finish(X_INIT, z, x)
                if not waited & {GAIN}:
                    waited.add(GAIN)
                    finish(GAIN, 0, gains.at[pl.ds(0, R - 1)])
            cos = cos_ref[z]
            sin = sin_ref[z]

            def head(i):
                return total(QKV_B, z, sbq, rbq, slice(i * HD, (i + 1) * HD))

            def rope(v):
                return (v * cos + pltpu.roll(v, HD // 2, 1) * sin).astype(BF16).astype(F32)

            seqs = slice(z * SZ, (z + 1) * SZ)
            for h in range(QH):
                v = rope(head(h))
                for s in range(STEPS):
                    qs[:, s * 8 + h, :] = v[s * SZ:(s + 1) * SZ]
            for h in range(KH):
                v = rope(head(QH + h))
                w = head(QH + KH + h)
                for s in range(STEPS):
                    kn_ref[l, seqs, s * KH + h, :] = v[s * SZ:(s + 1) * SZ]
                    vn_ref[l, seqs, s * KH + h, :] = w[s * SZ:(s + 1) * SZ]

            qall = qs[...].reshape(rows, HD).astype(BF16)
            knew = kn_ref[l, seqs].reshape(SZ * 8, HD).astype(BF16)
            vnew = vn_ref[l, seqs].reshape(SZ * 8, HD).astype(BF16)
            s_new = lax.dot_general(qall, knew, NT, preferred_element_type=F32) * sc
            sn[...] = jnp.where(new_ok, s_new, -jnp.inf).reshape(SZ, 16, SZ * 8)
            wwait(l, 3, 4)
            kvrow = jnp.where(lax.broadcasted_iota(jnp.int32, (16, SLOTS), 0) % 8 >= G, 1, 0)
            kcol = lax.broadcasted_iota(jnp.int32, (16, SLOTS), 1)
            parity = (kcol % KH) == kvrow

            def attend(b, carry):
                q = z * SZ + b
                s = lax.dot_general(qs[b].astype(BF16), ck[l, q], NT, preferred_element_type=F32) * sc
                s = jnp.where(parity & (kcol < len_ref[q] * KH), s, -jnp.inf)
                t = sn[b]
                m = jnp.maximum(jnp.max(s, axis=-1, keepdims=True), jnp.max(t, axis=-1, keepdims=True))
                e = jnp.exp(s - m)
                f = jnp.exp(t - m)
                den = jnp.sum(e, axis=-1, keepdims=True) + jnp.sum(f, axis=-1, keepdims=True)
                pn[b] = (f / den).astype(BF16)
                os[b] = jnp.dot((e / den).astype(BF16), cv[l, q], preferred_element_type=F32)
                return carry

            lax.fori_loop(0, SZ, attend, 0, unroll=4)
            o_new = jnp.dot(pn[...].reshape(rows, SZ * 8), vnew, preferred_element_type=F32)
            os[...] = os[...] + o_new.reshape(SZ, 16, HD)
            for h in range(QH):
                o = jnp.concatenate([os[:, s * 8 + h, :] for s in range(STEPS)], axis=0)
                ago[z, own + h // per, :, (h % per) * HD:(h % per + 1) * HD] = o.astype(BF16)
            gather_start(O_COL, z, ago)

        def o_row(z):
            gather_finish(O_COL, z, ago)
            spread_start(O_ROW, z, ago, no)

        def project(act, z, w, depth, ph):
            lhs = act[z].reshape(ALL, depth)
            for h in range(HALVES):
                put(sbo, z, slice(h * WB, (h + 1) * WB),
                    jnp.dot(lhs, w[l, :, h * WB:(h + 1) * WB], preferred_element_type=F32))
            sum_start(ph, z, sbo, pro, rbo)

        def out(z):
            spread_finish(O_ROW, z, no)
            wwait(l, 5)
            project(no, z, wo, WB, OUT_B)

        def residual(z, ph, ph_col):
            sum_finish(ph, z, sbo, rbo)
            for h in range(HALVES):
                a = total(ph, z, sbo, rbo, slice(h * WB, (h + 1) * WB))
                x[z, own + h] = (x[z, own + h].astype(F32) + a).astype(BF16)
            gather_start(ph_col, z, x)

        def mlp_norm(z):
            gather_finish(X_MID, z, x)
            norm(z, L + l, False)
            spread_start(N_MLP, z, ns, nb)

        def gate_up(z):
            spread_finish(N_MLP, z, nb)
            wwait(l, 6, 7)

            def body(t, carry):
                off = pl.multiple_of(t * tile, tile)
                n = nb[z].reshape(ALL, WB)
                for k, w in enumerate((wg, wu)):
                    put(sbg, z, pl.ds(off + k * FF, tile), jnp.dot(n, w[l, :, pl.ds(off, tile)], preferred_element_type=F32))
                return carry

            lax.fori_loop(0, FF // tile, body, 0)
            sum_start(GU_B, z, sbg, prg, rbg)

        def gate_up_middle(z):
            sum_middle(GU_B, z, sbg, prg, rbg, 8)

        def act(z):
            sum_finish(GU_B, z, sbg, rbg)
            per_half = half // tile

            def body(t, carry):
                off = pl.multiple_of(t * tile, tile)
                g = total(GU_B, z, sbg, rbg, pl.ds(off, tile))
                u = total(GU_B, z, sbg, rbg, pl.ds(off + FF, tile))
                aga[z, own + t // per_half, :, pl.ds(pl.multiple_of((t % per_half) * tile, tile), tile)] = (jax.nn.silu(g) * u).astype(BF16)
                return carry

            lax.fori_loop(0, FF // tile, body, 0)
            gather_start(A_COL, z, aga)

        def a_row(z):
            gather_finish(A_COL, z, aga)
            spread_start(A_ROW, z, aga, na)

        def down(z):
            spread_finish(A_ROW, z, na)
            wwait(l, 8)
            project(na, z, wd, half, DOWN_B)

        def end_norm(z):
            gather_finish(X_END, z, x)
            norm(z, l + 1, l == L - 1)
            spread_start(N_ATTN, z, ns, nb)

        stages = [qkv, attention, o_row, out]
        stages += [lambda z: sum_middle(OUT_B, z, sbo, pro, rbo, 1)] if PRE[OUT_B] is not None else []
        stages += [lambda z: residual(z, OUT_B, X_MID), mlp_norm, gate_up, gate_up_middle, act, a_row, down]
        stages += [lambda z: sum_middle(DOWN_B, z, sbo, pro, rbo, 1)] if PRE[DOWN_B] is not None else []
        stages += [lambda z: residual(z, DOWN_B, X_END), end_norm]
        return stages

    stages = [stage for l in range(L) for stage in layer_stages(l)]
    for i, z in stage_order(L):
        stages[i](z)
    for z in range(STREAMS):
        spread_finish(N_ATTN, z, nb)
    for b in range(R):
        v = [nb[z, b].astype(F32) for z in range(STREAMS)]
        for s, out in enumerate((out0, out1)):
            out[b * SEQ:(b + 1) * SEQ] = jnp.concatenate([w[s * SZ:(s + 1) * SZ] for w in v], axis=0).astype(BF16)


def cache_kernel(heads, len_ref, kn_ref, vn_ref, a0, a1, ck_ref, cv_ref, ok_ref, ov_ref, o0, o1,
                 kwin, vwin, bsem, wsem, nsem):
    layers, seqs, rows, width = ck_ref.shape
    sides = ((ck_ref, kwin, kn_ref, ok_ref), (cv_ref, vwin, vn_ref, ov_ref))
    pass_on = [pltpu.make_async_copy(a, b, nsem.at[i]) for i, (a, b) in enumerate(((a0, o0), (a1, o1)))]
    group = seqs // COPY_GROUPS

    def bulk(k, i):
        at = (i // COPY_GROUPS, pl.ds((i % COPY_GROUPS) * group, group))
        return pltpu.make_async_copy(sides[k][0].at[at], sides[k][3].at[at], bsem.at[k, i])

    def place(b):
        at = len_ref[b] * heads
        return at, pl.multiple_of(jnp.minimum((at // 16) * 16, rows - 32), 16)

    def window(k, layer, b):
        return pltpu.make_async_copy(sides[k][1].at[layer, b], sides[k][3].at[layer, b, pl.ds(place(b)[1], 32)], wsem.at[k, layer, b])

    count = layers * COPY_GROUPS
    for i in range(count):
        for k in range(2):
            bulk(k, i).start()
    for cp in pass_on:
        cp.start()

    def patch(b, carry):
        at, base = place(b)
        idx = lax.broadcasted_iota(jnp.int32, (32, width), 0) + base - at
        for layer in range(layers):
            for src, win, fresh, _ in sides:
                val = src[layer, b, pl.ds(base, 32), :].astype(F32)
                new = fresh[layer, b]
                for n in range(STEPS * heads):
                    val = jnp.where(idx == n, new[n:n + 1, :], val)
                win[layer, b] = val.astype(BF16)
        return carry

    lax.fori_loop(0, seqs, patch, 0, unroll=2)
    for i in range(count):
        for k in range(2):
            bulk(k, i).wait()
        for g in range(group):
            for k in range(2):
                window(k, i // COPY_GROUPS, (i % COPY_GROUPS) * group + g).start()
    for cp in pass_on:
        cp.wait()
    for layer in range(layers):
        for b in range(seqs):
            for k in range(2):
                window(k, layer, b).wait()


def solution(mesh):
    R, C = mesh.shape['row'], mesh.shape['col']
    hidden_spec = P('rep', 'row')
    index_spec = P(('rep', 'row'))
    cache_spec = P(None, ('rep', 'row'), None, 'col', None)
    gain_spec = P(None, 'row')
    weight_spec = P(None, 'row', 'col')

    def device_program(hidden_0, hidden_1, positions, lengths, cache_k, cache_v, norm_attn, norm_mlp, w_query, w_key, w_value, w_out, w_gate, w_up, w_down):
        L, SEQ, CTX, KH, HD = cache_k.shape
        WB = hidden_0.shape[1]
        SZ = SEQ // STREAMS
        TOK = SZ * STEPS
        XS = R // CORES
        Z = STREAMS
        QC, KC, FF = w_query.shape[-1], w_key.shape[-1], w_gate.shape[-1]
        HALVES = R // C
        SLOTS = CTX * KH
        ck = cache_k.reshape(L, SEQ, SLOTS, HD)
        cv = cache_v.reshape(L, SEQ, SLOTS, HD)
        vm = pl.BlockSpec(memory_space=pltpu.VMEM)
        smem = pl.BlockSpec(memory_space=pltpu.SMEM)
        hbm = pl.BlockSpec(memory_space=pltpu.HBM)
        weights = (w_query, w_key, w_value, w_out, w_gate, w_up, w_down)
        scratch = [pltpu.VMEM(w.shape, BF16) for w in weights]
        N3 = QC + 2 * KC
        N2 = 2 * FF
        OUTW = HALVES * WB

        def slots(ph):
            return R - 1 if PRE[ph] is None else XS - 1

        scratch += [pltpu.VMEM(s, d) for s, d in (
            ((Z, TOK, HD), F32), ((Z, TOK, HD), F32), ((8, WB), F32), ((8, 128), F32), ((R, 8, 128), F32),
            ((Z, R, TOK, WB), BF16), ((Z, R, TOK, WB), BF16), ((R, 8, WB), F32), ((Z, R, TOK, WB), BF16), ((Z, R, TOK, WB), BF16),
            ((Z, CORES, XS, TOK, N3), BF16), ((Z, XS, TOK, N3), BF16), ((Z, slots(QKV_B), TOK, N3), BF16),
            ((SZ, 16, HD), F32), ((SZ, 16, SZ * 8), F32), ((SZ, 16, SZ * 8), BF16), ((SZ, 16, HD), F32),
            ((Z, R, TOK, WB), BF16), ((Z, R, TOK, WB), BF16),
            ((Z, CORES, XS, TOK, OUTW), BF16), ((Z, XS, TOK, OUTW), BF16), ((Z, slots(OUT_B), TOK, OUTW), BF16),
            ((Z, CORES, XS, TOK, N2), BF16), ((Z, XS, TOK, N2), BF16), ((Z, slots(GU_B), TOK, N2), BF16),
            ((Z, R, TOK, FF // HALVES), BF16), ((Z, R, TOK, FF // HALVES), BF16))]
        scratch += [pltpu.SemaphoreType.DMA((PHASES, Z))] * 2 + [pltpu.SemaphoreType.DMA((L, 9))]
        dims = dict(R=R, C=C, L=L, D=WB * R, HD=HD)
        out_0, out_1, k_new, v_new, kept_k, kept_v = pl.pallas_call(
            functools.partial(decode_kernel, dims),
            out_shape=(pltpu.VMEM(hidden_0.shape, BF16), pltpu.VMEM(hidden_1.shape, BF16),
                       pltpu.VMEM((L, SEQ, 8, HD), F32), pltpu.VMEM((L, SEQ, 8, HD), F32),
                       pltpu.VMEM(ck.shape, BF16), pltpu.VMEM(ck.shape, BF16)),
            in_specs=[vm, vm, smem, smem, vm, vm] + [hbm] * 9,
            out_specs=(vm,) * 6,
            scratch_shapes=scratch,
            compiler_params=pltpu.CompilerParams(collective_id=0, has_side_effects=True, vmem_limit_bytes=47 * 1024 * 1024),
            name='decode',
        )(hidden_0, hidden_1, positions, lengths, norm_attn, norm_mlp, *weights, ck, cv)

        count = L * COPY_GROUPS
        win = pltpu.VMEM((L, SEQ, 32, HD), BF16)
        ok, ov, out_0, out_1 = pl.pallas_call(
            functools.partial(cache_kernel, KH),
            out_shape=(jax.ShapeDtypeStruct(ck.shape, BF16),) * 2 + (jax.ShapeDtypeStruct(hidden_0.shape, BF16),) * 2,
            in_specs=[smem] + [vm] * 6,
            out_specs=(hbm,) * 4,
            scratch_shapes=[win, win, pltpu.SemaphoreType.DMA((2, count)),
                            pltpu.SemaphoreType.DMA((2, L, SEQ)), pltpu.SemaphoreType.DMA((2,))],
            compiler_params=pltpu.CompilerParams(vmem_limit_bytes=8 * 1024 * 1024),
            name='cache_update',
        )(lengths, k_new, v_new, out_0, out_1, kept_k, kept_v)
        ok, ov = ok.reshape(cache_k.shape), ov.reshape(cache_v.shape)
        return out_0, out_1, ok, ov

    return jax.shard_map(device_program, mesh=mesh,
                         in_specs=(hidden_spec, hidden_spec, index_spec, index_spec, cache_spec, cache_spec, gain_spec, gain_spec) + (weight_spec,) * 7,
                         out_specs=(hidden_spec, hidden_spec, cache_spec, cache_spec), check_vma=False)
```
